32 devices in a mesh: dp: 8 (over z, y), vocab: 4 (over x, core).
Axes of the slice: x: 2, y: 2, z: 4, core: 2. Of those that a mesh axis runs over, the one named last changes fastest.
Arguments:
- hidden_states: bfloat16 [4096, 2048], P('dp', 'vocab'), may hold values from -12 to 12
- teacher_logits: bfloat16 [4096, 16384], P('dp', 'vocab'), may hold values from -24 to 240
- head_weight: bfloat16 [2048, 16384], P(None, 'vocab'), as said below
Outputs:
- kl_per_token: float32 [4096], P('dp')
- hidden_grad: bfloat16 [4096, 2048], P('dp', 'vocab')
- head_grad: float32 [2048, 16384], P('dp', 'vocab')
The draws below stay inside these ranges and needn't reach their ends.
Inputs may be any that keep to these rules, and one draw needn't show every extreme that they name: `head_weight`: every entry's magnitude is at most 18 / sqrt(2048).
All inputs are finite; a program needn't handle non-finite values.
Results may differ from the reference program's by a relative error of at most 0.014.
Values may be sent and summed in bfloat16 or wider, within the bound.
A program may use at most 128 MiB of HBM per device.

```python
import math
import jax
import jax.numpy as jnp
from jax import lax

D = 2048
V = 16384
MICRO = 2
TOK = 256
TOKENS = 4096
N_DP = 8


def head_columns(key):
    column_key = jax.random.fold_in(key, 7101)
    value_key = jax.random.fold_in(column_key, 1)
    spread = 3.0 / math.sqrt(D)
    values = jnp.clip(jax.random.normal(value_key, (D, V), jnp.float32), -6.0, 6.0)
    return values * spread


def draw_head_weight(key, part):
    return head_columns(key).astype(jnp.bfloat16)


def draw_hidden_states(key, part):
    streams = jax.random.split(jax.random.fold_in(key, 7202), 2)
    values = jnp.clip(jax.random.normal(streams[1], (TOKENS, D), jnp.float32), -6.0, 6.0)
    return values.astype(jnp.bfloat16)


def draw_teacher_logits(key, part):
    streams = jax.random.split(jax.random.fold_in(key, 7303), 3)
    values = 3.0 * jnp.clip(jax.random.normal(streams[2], (TOKENS, V), jnp.float32), -8.0, 8.0)
    return values.astype(jnp.bfloat16)


def setup_inputs(seed: int = 0) -> dict:
    key_list = jax.random.split(jax.random.key(seed), 4)
    hidden_states = draw_hidden_states(jax.random.fold_in(key_list[3], 71), 0)
    teacher_logits = draw_teacher_logits(jax.random.fold_in(key_list[3], 71), 0)
    head_weight = draw_head_weight(jax.random.fold_in(key_list[3], 71), 0)
    return {"hidden_states": hidden_states, "teacher_logits": teacher_logits, "head_weight": head_weight}


grad_scale = 8.0


def token_group(hidden_rows, teacher_rows, head_weight):
    student = jnp.dot(hidden_rows, head_weight, preferred_element_type=jnp.float32)
    teacher = teacher_rows.astype(jnp.float32)
    student_max = jnp.max(student, axis=1, keepdims=True)
    teacher_max = jnp.max(teacher, axis=1, keepdims=True)
    student_terms = jnp.exp(student - student_max)
    teacher_terms = jnp.exp(teacher - teacher_max)
    student_total = jnp.sum(student_terms, axis=1)
    teacher_total = jnp.sum(teacher_terms, axis=1)
    cross_term = jnp.sum(teacher_terms * (teacher - student), axis=1)
    divergence = cross_term / teacher_total - teacher_max[:, 0] - jnp.log(teacher_total) + student_max[:, 0] + jnp.log(student_total)
    logit_grad = (grad_scale * (student_terms / student_total[:, None] - teacher_terms / teacher_total[:, None])).astype(jnp.bfloat16)
    hidden_grad = lax.dot_general(logit_grad, head_weight, (((1,), (1,)), ((), ())), preferred_element_type=jnp.float32).astype(jnp.bfloat16)
    group_grad = lax.dot_general(hidden_rows, logit_grad, (((0,), (0,)), ((), ())), preferred_element_type=jnp.float32).astype(jnp.bfloat16)
    return divergence, hidden_grad, group_grad


def reference(hidden_states, teacher_logits, head_weight):
    group_rows = MICRO * TOK
    grouped_hidden = hidden_states.reshape(N_DP, group_rows, D)
    grouped_teacher = teacher_logits.reshape(N_DP, group_rows, V)

    def one_group(running, inputs):
        divergence, hidden_grad, group_grad = token_group(inputs[0], inputs[1], head_weight)
        running = running + lax.optimization_barrier(group_grad).astype(jnp.float32)
        return running, (divergence, hidden_grad)

    head_grad, results = lax.scan(one_group, jnp.zeros((D, V), jnp.float32), (grouped_hidden, grouped_teacher))
    divergence = results[0].reshape(TOKENS)
    hidden_grad = results[1].reshape(TOKENS, D)
    return divergence, hidden_grad, head_grad
```

```python
import functools

import jax
import jax.numpy as jnp
from jax import lax
from jax.experimental import pallas as pl
from jax.experimental.pallas import tpu as pltpu
from jax.sharding import PartitionSpec as P

grad_scale = 8.0
PAIR = 2
CORES = 2
LANES = 128
MESH = pl.DeviceIdType.MESH
f32 = jnp.float32
bf16 = jnp.bfloat16


class Plan:
    def __init__(self, shards, vocab, tokens, shard, model_width, columns):
        self.line = shards // PAIR
        self.vocab = vocab
        self.chips = vocab // CORES
        self.tokens = tokens
        self.shard = shard
        self.model_width = model_width
        self.columns = columns
        self.halves = 2
        self.half_tokens = tokens // self.halves
        self.half = columns // PAIR
        self.width = min(256, self.half)
        self.chunks = self.half // self.width
        self.rows2 = model_width // self.line
        self.rows = self.rows2 // PAIR
        self.window = min(3, self.chunks)
        self.lag = min(2, self.chunks)
        self.end_lag = self.lag + 2
        self.last_lag = self.end_lag + 1
        self.ahead = min(2, self.chunks)
        self.hid_width = min(256, shard)
        self.hid_subs = shard // self.hid_width
        self.hid_blocks = vocab * self.hid_subs
        self.slots = 2 if self.line == 4 else self.line + 1


def fused_kernel(
    plan,
    hidden_ref, teacher_ref, weight_ref,
    kl_ref, hid_ref, out_ref,
    weight, student, grad, gathered, features, pair_grad, incoming, outgoing, block,
    pair_out, pair_in, hid_out, hid_in, hid_far_out, hid_far_in, hid_sum,
    row_student, row_teacher, lane_stats, stats,
    load_sem, weight_sem, out_sem,
    gather_send, gather_recv, fy_send, fy_recv, fz_send, fz_recv, fx_send, fx_recv, fc_send, fc_recv,
    stat_send, stat_recv, y_send, y_recv, zo_send, zo_recv, zf_send, zf_recv,
    line_send, line_recv, last_send, last_recv,
    hc_send, hc_recv, hx_send, hx_recv,
):
    line, vocab, chips = plan.line, plan.vocab, plan.chips
    tokens, shard, half, width, chunks = plan.tokens, plan.shard, plan.half, plan.width, plan.chunks
    rows2, rows, half_tokens = plan.rows2, plan.rows, plan.half_tokens
    columns = plan.columns

    me = lax.axis_index("dp")
    v = lax.axis_index("vocab")
    place = me // PAIR
    side = me - place * PAIR
    partner = place * PAIR + (PAIR - 1) - side
    chip = v // CORES
    core = v - chip * CORES
    other_core = chip * CORES + (CORES - 1) - core
    has_down = place > 0
    has_up = place < line - 1
    up = jnp.where(has_up, me + PAIR, me)
    down = jnp.where(has_down, me - PAIR, me)
    is_low = place == 0
    is_high = place == line - 1
    is_end = jnp.logical_or(is_low, is_high)
    next_low = place == 1
    next_high = place == line - 2
    is_next = jnp.logical_or(next_low, next_high)
    inner = jnp.where(is_low, up, down)

    def chip_after(step):
        return lax.rem(chip + step, chips)

    def chip_before(step):
        return lax.rem(chip + chips - step, chips)

    def shard_of(index):
        return pl.ds(pl.multiple_of(index * shard, shard), shard)

    def chip_rows(index):
        return pl.ds(pl.multiple_of(index * CORES * shard, CORES * shard), CORES * shard)

    def token_half(part):
        return pl.ds(part * half_tokens, half_tokens)

    def columns_of(chunk):
        return pl.ds(pl.multiple_of(chunk * width, width), width)

    def grad_columns(which, chunk):
        return pl.ds(pl.multiple_of(which * half + chunk * width, width), width)

    def remote(src, dst, send, recv, **target):
        return pltpu.make_async_remote_copy(
            src_ref=src, dst_ref=dst, send_sem=send, recv_sem=recv, device_id=target, device_id_type=MESH
        )

    own_load = pltpu.make_async_copy(hidden_ref, gathered.at[:, shard_of(v)], load_sem.at[0])
    teacher_load = pltpu.make_async_copy(teacher_ref, grad, load_sem.at[1])

    def weight_load(step):
        part = chip_rows(chip_before(step))
        return pltpu.make_async_copy(weight_ref.at[part, :], weight.at[part, :], weight_sem.at[step])

    barrier = pltpu.get_barrier_semaphore()
    for step in range(1, vocab):
        pl.semaphore_signal(
            barrier, inc=1, device_id={"vocab": lax.rem(v + step, vocab)}, device_id_type=MESH
        )
    pl.semaphore_signal(barrier, inc=1, device_id={"dp": partner}, device_id_type=MESH)

    @pl.when(has_down)
    def _():
        pl.semaphore_signal(barrier, inc=1, device_id={"dp": down}, device_id_type=MESH)

    @pl.when(has_up)
    def _():
        pl.semaphore_signal(barrier, inc=1, device_id={"dp": up}, device_id_type=MESH)

    own_load.start()
    weight_load(0).start()
    teacher_load.start()
    for step in range(1, chips):
        weight_load(step).start()
    own_load.wait()
    pl.semaphore_wait(barrier, vocab + has_down.astype(jnp.int32) + has_up.astype(jnp.int32))

    def gather_copy(index, part, column, target):
        ref = gathered.at[token_half(part), shard_of(column)]
        return remote(ref, ref, gather_send.at[index, part], gather_recv.at[index, part], vocab=target)

    def gather_far(step, part):
        return gather_copy(step, part, v, chip_after(step) * CORES + core)

    def gather_pass(step, part):
        return gather_copy(chips - 1 + step, part, chip_before(step) * CORES + core, other_core)

    for part in range(plan.halves):
        for step in range(1, chips):
            gather_far(step, part).start()
        gather_copy(0, part, v, other_core).start()

    def set_ref(which, index):
        return features.at[shard_of(index), pl.ds(which * tokens, tokens)]

    def turn(index):
        features[shard_of(index), 0:tokens] = gathered[:, shard_of(index)].T

    def feature_y(step):
        index = chip_before(step) * CORES + core
        return remote(set_ref(0, index), set_ref(1, index), fy_send.at[step], fy_recv.at[step], dp=partner)

    def feature_z(which):
        return remote(set_ref(which, v), set_ref(2 + which, v), fz_send.at[which], fz_recv.at[which], dp=inner)

    def feature_x(which, step):
        ref = set_ref(which, v)
        return remote(
            ref, ref, fx_send.at[which - 2, step], fx_recv.at[which - 2, step],
            vocab=chip_after(step) * CORES + core,
        )

    def feature_core(which, step):
        ref = set_ref(which, chip_before(step) * CORES + core)
        return remote(ref, ref, fc_send.at[which - 1, step], fc_recv.at[which - 1, step], vocab=other_core)

    turn(v)
    feature_y(0).start()

    @pl.when(is_end)
    def _():
        feature_z(0).start()

    for part in range(plan.halves):
        gather_copy(0, part, other_core, other_core).wait_recv()
    weight_load(0).wait()
    dot_width = min(512, columns)

    @pl.loop(0, columns // dot_width)
    def _(index):
        where = pl.ds(pl.multiple_of(index * dot_width, dot_width), dot_width)
        student[:, where] = jnp.dot(
            gathered[:, chip_rows(chip)], weight[chip_rows(chip), where], preferred_element_type=f32
        )

    teacher_load.wait()
    band = 32

    @pl.loop(0, tokens // band)
    def _(index):
        where = pl.ds(pl.multiple_of(index * band, band), band)
        top = grad[where, 0:LANES]
        for column in range(1, columns // LANES):
            top = jnp.maximum(top, grad[where, column * LANES : (column + 1) * LANES])
        lane_stats[0, where, :] = top.astype(f32)

    row_teacher[...] = jnp.broadcast_to(jnp.max(lane_stats[0], axis=1, keepdims=True), (tokens, LANES))
    turn(other_core)

    def stat_copy(step, part, owner, target):
        ref = stats.at[owner, :, token_half(part)]
        return remote(ref, ref, stat_send.at[step, part], stat_recv.at[step, part], vocab=target)

    def first_half(part):
        where_rows = token_half(part)
        for step in range(1, chips):
            gather_copy(step, part, chip_before(step) * CORES + core, other_core).wait_recv()
            gather_pass(step, part).start()
        for step in range(1, chips):
            gather_copy(
                chips - 1 + step, part, chip_before(step) * CORES + (CORES - 1) - core, other_core
            ).wait_recv()
        if part == 0:
            for step in range(1, chips):
                weight_load(step).wait()
        lane_stats[0, where_rows, :] = jnp.full((half_tokens, LANES), -jnp.inf, f32)

        @pl.loop(0, columns // dot_width)
        def _(index):
            where = pl.ds(pl.multiple_of(index * dot_width, dot_width), dot_width)
            total = student[where_rows, where]
            for step in range(1, chips):
                far = chip_rows(chip_before(step))
                total = total + jnp.dot(
                    gathered[where_rows, far], weight[far, where], preferred_element_type=f32
                )
            student[where_rows, where] = total
            top = lane_stats[0, where_rows, :]
            for column in range(dot_width // LANES):
                top = jnp.maximum(top, total[:, column * LANES : (column + 1) * LANES])
            lane_stats[0, where_rows, :] = top

        student_top = jnp.max(lane_stats[0, where_rows, :], axis=1, keepdims=True)
        row_student[where_rows, :] = jnp.broadcast_to(student_top, (half_tokens, LANES))

        @pl.loop(0, half_tokens // band)
        def _(index):
            where = pl.ds(pl.multiple_of(part * half_tokens + index * band, band), band)
            student_max, teacher_max = row_student[where, :], row_teacher[where, :]
            sums = [jnp.zeros((band, LANES), f32) for _ in range(3)]
            for column in range(columns // LANES):
                lanes = slice(column * LANES, (column + 1) * LANES)
                logit, target = student[where, lanes], grad[where, lanes].astype(f32)
                term = jnp.exp(target - teacher_max)
                sums[0] += jnp.exp(logit - student_max)
                sums[1] += term
                sums[2] += term * (target - logit)
            for which in range(3):
                lane_stats[which, where, :] = sums[which]

        lane = lax.broadcasted_iota(jnp.int32, (half_tokens, LANES), 1)
        packed = jnp.where(lane == 0, row_student[where_rows, :], row_teacher[where_rows, :])
        for which in range(3):
            total = jnp.sum(lane_stats[which, where_rows, :], axis=1, keepdims=True)
            packed = jnp.where(lane == 2 + which, jnp.broadcast_to(total, packed.shape), packed)
        stats[v, :, where_rows] = packed.T[0:8, :]
        for step in range(1, vocab):
            stat_copy(step, part, v, lax.rem(v + step, vocab)).start()

    def y_copy(part, chunk):
        return remote(
            grad.at[token_half(part), grad_columns(PAIR - 1 - side, chunk)],
            pair_grad.at[token_half(part), columns_of(chunk)],
            y_send.at[part, chunk], y_recv.at[part, chunk], dp=partner,
        )

    def end_own(part, chunk):
        return remote(
            grad.at[token_half(part), grad_columns(side, chunk)],
            pair_grad.at[pl.ds(tokens + part * half_tokens, half_tokens), columns_of(chunk)],
            zo_send.at[part, chunk], zo_recv.at[part, chunk], dp=inner,
        )

    def end_pair(part, chunk):
        return remote(
            pair_grad.at[token_half(part), columns_of(chunk)],
            pair_grad.at[pl.ds(2 * tokens + part * half_tokens, half_tokens), columns_of(chunk)],
            zf_send.at[part, chunk], zf_recv.at[part, chunk], dp=inner,
        )

    def second_half(part):
        where_rows = token_half(part)
        for step in range(1, vocab):
            stat_copy(step, part, lax.rem(v + vocab - step, vocab), other_core).wait_recv()
        parts = [stats[index, :, where_rows] for index in range(vocab)]
        student_max = functools.reduce(jnp.maximum, [p[0:1] for p in parts])
        teacher_max = functools.reduce(jnp.maximum, [p[1:2] for p in parts])
        student_total = sum(p[2:3] * jnp.exp(p[0:1] - student_max) for p in parts)
        teacher_scales = [jnp.exp(p[1:2] - teacher_max) for p in parts]
        teacher_total = sum(p[3:4] * scale for p, scale in zip(parts, teacher_scales))
        cross = sum(p[4:5] * scale for p, scale in zip(parts, teacher_scales))
        student_log = student_max + jnp.log(student_total)
        teacher_log = teacher_max + jnp.log(teacher_total)
        kl_ref[:, where_rows] = cross / teacher_total - teacher_log + student_log
        row = lax.broadcasted_iota(jnp.int32, (LANES, half_tokens), 0)
        packed = jnp.where(
            row == 0,
            jnp.broadcast_to(student_log, (LANES, half_tokens)),
            jnp.broadcast_to(teacher_log, (LANES, half_tokens)),
        ).T
        row_student[where_rows, :] = jnp.broadcast_to(packed[:, 0:1], (half_tokens, LANES))
        row_teacher[where_rows, :] = jnp.broadcast_to(packed[:, 1:2], (half_tokens, LANES))

        @pl.loop(0, half_tokens // band)
        def _(index):
            where = pl.ds(pl.multiple_of(part * half_tokens + index * band, band), band)
            student_row, teacher_row = row_student[where, :], row_teacher[where, :]
            for column in range(columns // LANES):
                lanes = slice(column * LANES, (column + 1) * LANES)
                value = jnp.exp(student[where, lanes] - student_row) - jnp.exp(
                    grad[where, lanes].astype(f32) - teacher_row
                )
                grad[where, lanes] = (grad_scale * value).astype(bf16)

        @pl.loop(0, chunks)
        def _(chunk):
            y_copy(part, chunk).start()

        @pl.when(is_end)
        def _():
            for chunk in range(plan.ahead):
                end_own(part, chunk).start()

    def first_service():
        feature_y(0).wait_recv()
        feature_core(1, 0).start()

        @pl.when(is_end)
        def _():
            feature_z(1).start()

        @pl.when(is_next)
        def _():
            feature_z(0).wait_recv()
            for step in range(1, chips):
                feature_x(2, step).start()
            feature_core(2, 0).start()

        for step in range(1, chips):
            turn(chip_before(step) * CORES + core)
            feature_y(step).start()
        for step in range(1, chips):
            turn(chip_before(step) * CORES + (CORES - 1) - core)

    def second_service():
        for step in range(1, chips):
            feature_y(step).wait_recv()
            feature_core(1, step).start()

        @pl.when(is_next)
        def _():
            feature_z(1).wait_recv()
            for step in range(1, chips):
                feature_x(3, step).start()
            feature_core(3, 0).start()
            for which in (2, 3):
                for step in range(1, chips):
                    feature_x(which, step).wait_recv()
                    feature_core(which, step).start()
            for which in (2, 3):
                for step in range(chips):
                    feature_core(which, step).wait_recv()

        for step in range(chips):
            feature_core(1, step).wait_recv()

    first_half(0)
    first_half(1)
    second_half(0)
    first_service()
    second_half(1)
    second_service()

    def hid_core(index):
        return remote(
            hid_out.at[index], hid_in.at[index], hc_send.at[index], hc_recv.at[index], vocab=other_core
        )

    def hid_far(index):
        return remote(
            hid_far_out.at[index], hid_far_in.at[index], hx_send.at[index], hx_recv.at[index],
            vocab=lax.rem(chip + 1 + index, chips) * CORES + core,
        )

    def hid_block(index):
        piece = index // plan.hid_subs
        sub = index - piece * plan.hid_subs
        mine = piece >= chips
        order = jnp.where(mine, piece - chips, piece)
        target = lax.rem(chip + 1 + order, chips) * CORES + jnp.where(mine, core, (CORES - 1) - core)
        where = pl.ds(pl.multiple_of(target * shard + sub * plan.hid_width, plan.hid_width), plan.hid_width)
        lanes = pl.ds(pl.multiple_of(sub * plan.hid_width, plan.hid_width), plan.hid_width)
        last_sub = sub == plan.hid_subs - 1
        value = lax.dot_general(
            grad[...], weight[where, :], (((1,), (1,)), ((), ())), preferred_element_type=f32
        )

        @pl.when(jnp.logical_not(mine))
        def _():
            hid_out[order, :, lanes] = value.astype(bf16)

            @pl.when(last_sub)
            def _():
                hid_core(order).start()

        @pl.when(mine)
        def _():
            @pl.when(sub == 0)
            def _():
                hid_core(order).wait_recv()

            total = value + hid_in[order, :, lanes].astype(f32)

            @pl.when(order < chips - 1)
            def _():
                hid_far_out[order, :, lanes] = total.astype(bf16)

                @pl.when(last_sub)
                def _():
                    hid_far(order).start()

            @pl.when(order == chips - 1)
            def _():
                hid_sum[:, lanes] = total

    def rows_of(part):
        return pl.ds(pl.multiple_of(part * rows2, rows2), rows2)

    def sum_into_block(part, chunk, with_end):
        where = columns_of(chunk)
        block[...] = jnp.dot(
            features[rows_of(part), 0:tokens], grad[:, grad_columns(side, chunk)], preferred_element_type=f32
        ) + jnp.dot(
            features[rows_of(part), tokens : 2 * tokens], pair_grad[0:tokens, where], preferred_element_type=f32
        )

        def add_end():
            block[...] += jnp.dot(
                features[rows_of(part), 2 * tokens : 4 * tokens],
                pair_grad[tokens : 3 * tokens, where],
                preferred_element_type=f32,
            )

        if with_end is True:
            add_end()
        elif with_end is not False:
            pl.when(with_end)(add_end)

    def base_slot(where):
        return jnp.where(jnp.logical_and(where >= 1, where <= line - 3), where + 1, 0)

    def line_copy(chunk, part, slot, target):
        return remote(
            outgoing.at[lax.rem(chunk, plan.window), part],
            incoming.at[slot, :, columns_of(chunk)],
            line_send.at[part, chunk], line_recv.at[slot, chunk], dp=target,
        )

    def send_sum(chunk, part, target, slot, source):
        @pl.when(chunk >= plan.window)
        def _():
            line_copy(chunk - plan.window, part, slot, target).wait_send()

        spot = lax.rem(chunk, plan.window)
        if source is None:
            outgoing[spot, part] = block[...].astype(bf16)
        else:
            has_source, source_slot = source

            @pl.when(has_source)
            def _():
                line_copy(chunk, part, source_slot, target).wait_recv()
                outgoing[spot, part] = (
                    block[...] + incoming[source_slot, :, columns_of(chunk)].astype(f32)
                ).astype(bf16)

            @pl.when(jnp.logical_not(has_source))
            def _():
                outgoing[spot, part] = block[...].astype(bf16)

        line_copy(chunk, part, slot, target).start()

    def up_slot(part):
        return base_slot(place + 1) + part - place - 1

    from_below = jnp.logical_and(place >= 2, jnp.logical_not(is_low))
    from_above = place <= line - 3

    def last_copy(chunk):
        return remote(
            pair_out.at[:, columns_of(chunk)], pair_in.at[:, columns_of(chunk)],
            last_send.at[chunk], last_recv.at[chunk], dp=partner,
        )

    def add_incoming(chunk, slot):
        line_copy(chunk, 0, slot, me).wait_recv()
        block[...] += incoming[slot, :, columns_of(chunk)].astype(f32)

    def settle(chunk):
        student[0:rows, grad_columns(side, chunk)] = block[
            pl.ds(pl.multiple_of(side * rows, rows), rows), :
        ]
        pair_out[:, columns_of(chunk)] = block[
            pl.ds(pl.multiple_of((PAIR - 1 - side) * rows, rows), rows), :
        ].astype(bf16)
        last_copy(chunk).start()

    def result_copy(which, chunk):
        spot = grad_columns(jnp.where(which == 0, side, PAIR - 1 - side), chunk)
        return pltpu.make_async_copy(student.at[0:rows, spot], out_ref.at[:, spot], out_sem.at[which, chunk])

    def early_sums(chunk):
        @pl.loop(0, line - 2)
        def _(index):
            part = jnp.where(next_low, line - 1 - index, index)
            sum_into_block(part, chunk, True)
            send_sum(
                chunk, part, jnp.where(next_low, up, down), jnp.where(next_low, up_slot(part), part), None
            )

    def late_sums(chunk):
        @pl.when(place >= 2)
        def _():
            @pl.loop(0, line - 1 - place)
            def _(index):
                part = line - 1 - index
                sum_into_block(part, chunk, False)
                send_sum(chunk, part, up, up_slot(part), (from_below, base_slot(place) + part - place))

        @pl.when(place <= line - 3)
        def _():
            @pl.loop(0, place)
            def _(part):
                sum_into_block(part, chunk, False)
                send_sum(chunk, part, down, part, (from_above, part))

        sum_into_block(place, chunk, is_next)

        @pl.when(from_below)
        def _():
            add_incoming(chunk, base_slot(place))

        @pl.when(from_above)
        def _():
            add_incoming(chunk, place)

        settle(chunk)

    @pl.loop(0, chunks + plan.last_lag)
    def _(step):
        @pl.when(step < plan.hid_blocks)
        def _():
            hid_block(step)

        @pl.when(step < chunks)
        def _():
            for part in range(plan.halves):
                y_copy(part, step).wait_recv()

            @pl.when(is_end)
            def _():
                for part in range(plan.halves):
                    end_pair(part, step).start()

                @pl.when(step + plan.ahead < chunks)
                def _():
                    for part in range(plan.halves):
                        end_own(part, step + plan.ahead).start()

            @pl.when(is_next)
            def _():
                for part in range(plan.halves):
                    end_own(part, step).wait_recv()
                    end_pair(part, step).wait_recv()
                early_sums(step)

        @pl.when(
            jnp.logical_and(
                jnp.logical_not(is_end),
                jnp.logical_and(step >= plan.lag, step < chunks + plan.lag),
            )
        )
        def _():
            late_sums(step - plan.lag)

        @pl.when(
            jnp.logical_and(is_end, jnp.logical_and(step >= plan.end_lag, step < chunks + plan.end_lag))
        )
        def _():
            chunk = step - plan.end_lag
            sum_into_block(place, chunk, False)
            add_incoming(chunk, 0)
            settle(chunk)

        @pl.when(step >= plan.last_lag)
        def _():
            chunk = step - plan.last_lag
            last_copy(chunk).wait_recv()
            student[0:rows, grad_columns(PAIR - 1 - side, chunk)] = pair_in[:, columns_of(chunk)].astype(f32)
            result_copy(0, chunk).start()
            result_copy(1, chunk).start()

    @pl.loop(min(chunks + plan.last_lag, plan.hid_blocks), plan.hid_blocks)
    def _(index):
        hid_block(index)

    total = hid_sum[...]
    for index in range(chips - 1):
        hid_far(index).wait_recv()
        total = total + hid_far_in[index].astype(f32)
    hid_ref[...] = total.astype(bf16)

    for part in range(plan.halves):
        for step in range(1, chips):
            gather_far(step, part).wait_send()
            gather_pass(step, part).wait_send()
        gather_copy(0, part, v, other_core).wait_send()
        for step in range(1, vocab):
            stat_copy(step, part, v, lax.rem(v + step, vocab)).wait_send()
    for step in range(chips):
        feature_y(step).wait_send()
        feature_core(1, step).wait_send()
        hid_core(step).wait_send()
    for index in range(chips - 1):
        hid_far(index).wait_send()

    @pl.when(is_end)
    def _():
        for which in range(2):
            feature_z(which).wait_send()

        @pl.loop(0, chunks)
        def _(chunk):
            for part in range(plan.halves):
                end_own(part, chunk).wait_send()
                end_pair(part, chunk).wait_send()

    @pl.when(is_next)
    def _():
        for which in (2, 3):
            feature_core(which, 0).wait_send()
            for step in range(1, chips):
                feature_x(which, step).wait_send()
                feature_core(which, step).wait_send()

    @pl.loop(0, chunks)
    def _(chunk):
        for part in range(plan.halves):
            y_copy(part, chunk).wait_send()
        last_copy(chunk).wait_send()
        result_copy(0, chunk).wait()
        result_copy(1, chunk).wait()

    @pl.when(jnp.logical_not(is_end))
    def _():
        @pl.loop(chunks - plan.window, chunks)
        def _(chunk):
            @pl.loop(0, place)
            def _(part):
                line_copy(chunk, part, 0, down).wait_send()

            @pl.loop(place + 1, line)
            def _(part):
                line_copy(chunk, part, 0, up).wait_send()


def per_device(shards, vocab, hidden_states, teacher_logits, head_weight):
    tokens, shard = hidden_states.shape
    model_width, columns = head_weight.shape
    plan = Plan(shards, vocab, tokens, shard, model_width, columns)
    dma = pltpu.SemaphoreType.DMA
    chips, halves, chunks = plan.chips, plan.halves, plan.chunks
    any_space = pl.BlockSpec(memory_space=pl.ANY)
    in_vmem = pl.BlockSpec(memory_space=pltpu.VMEM)
    divergence, hidden_grad, head_grad = pl.pallas_call(
        functools.partial(fused_kernel, plan),
        out_shape=(
            jax.ShapeDtypeStruct((1, tokens), f32),
            jax.ShapeDtypeStruct((tokens, shard), bf16),
            jax.ShapeDtypeStruct((plan.rows, columns), f32),
        ),
        in_specs=[any_space] * 3,
        out_specs=(in_vmem, in_vmem, any_space),
        scratch_shapes=[
            pltpu.VMEM((model_width, columns), bf16),
            pltpu.VMEM((tokens, columns), f32),
            pltpu.VMEM((tokens, columns), bf16),
            pltpu.VMEM((tokens, model_width), bf16),
            pltpu.VMEM((model_width, 4 * tokens), bf16),
            pltpu.VMEM((3 * tokens, plan.half), bf16),
            pltpu.VMEM((plan.slots, plan.rows2, plan.half), bf16),
            pltpu.VMEM((plan.window, plan.line, plan.rows2, plan.width), bf16),
            pltpu.VMEM((plan.rows2, plan.width), f32),
            pltpu.VMEM((plan.rows, plan.half), bf16),
            pltpu.VMEM((plan.rows, plan.half), bf16),
            pltpu.VMEM((chips, tokens, shard), bf16),
            pltpu.VMEM((chips, tokens, shard), bf16),
            pltpu.VMEM((chips - 1, tokens, shard), bf16),
            pltpu.VMEM((chips - 1, tokens, shard), bf16),
            pltpu.VMEM((tokens, shard), f32),
            pltpu.VMEM((tokens, LANES), f32),
            pltpu.VMEM((tokens, LANES), f32),
            pltpu.VMEM((3, tokens, LANES), f32),
            pltpu.VMEM((vocab, 8, tokens), f32),
            dma((2,)), dma((chips,)), dma((2, chunks)),
            dma((2 * chips - 1, halves)), dma((2 * chips - 1, halves)),
            dma((chips,)), dma((chips,)),
            dma((2,)), dma((2,)),
            dma((2, chips)), dma((2, chips)),
            dma((3, chips)), dma((3, chips)),
            dma((vocab, halves)), dma((vocab, halves)),
            dma((halves, chunks)), dma((halves, chunks)),
            dma((halves, chunks)), dma((halves, chunks)),
            dma((halves, chunks)), dma((halves, chunks)),
            dma((plan.line, chunks)), dma((plan.slots, chunks)),
            dma((chunks,)), dma((chunks,)),
            dma((chips,)), dma((chips,)),
            dma((chips - 1,)), dma((chips - 1,)),
        ],
        compiler_params=pltpu.CompilerParams(
            collective_id=0, has_side_effects=True, vmem_limit_bytes=67043328
        ),
    )(hidden_states, teacher_logits, head_weight)
    return divergence.reshape(tokens), hidden_grad, head_grad


def solution(mesh):
    in_specs = (P("dp", "vocab"), P("dp", "vocab"), P(None, "vocab"))
    out_specs = (P("dp"), P("dp", "vocab"), P("dp", "vocab"))
    return jax.shard_map(
        functools.partial(per_device, mesh.shape["dp"], mesh.shape["vocab"]),
        mesh=mesh, in_specs=in_specs, out_specs=out_specs, check_vma=False,
    )
```

```python
import functools
import math

import jax
import jax.numpy as jnp
from jax import lax
from jax.experimental import pallas as pl
from jax.experimental.pallas import tpu as pltpu
from jax.sharding import PartitionSpec as P

grad_scale = 8.0
PAIR = 2
CORES = 2
LANES = 128
MESH = pl.DeviceIdType.MESH
f32 = jnp.float32
bf16 = jnp.bfloat16


class Plan:
    def __init__(self, shards, vocab, tokens, shard, model_width, columns):
        self.line = shards // PAIR
        self.vocab = vocab
        self.chips = vocab // CORES
        self.tokens = tokens
        self.shard = shard
        self.model_width = model_width
        self.columns = columns
        self.halves = 2
        self.half_tokens = tokens // self.halves
        self.half = columns // PAIR
        self.width = min(256, self.half)
        self.chunks = self.half // self.width
        self.rows2 = model_width // self.line
        self.rows = self.rows2 // PAIR
        self.window = min(3, self.chunks)
        self.dot_width = min(512, columns)
        self.lag = min(2, self.chunks)
        self.end_lag = self.lag + 2
        self.last_lag = self.end_lag + 1
        self.ahead = min(2, self.chunks)
        self.first = min(2, self.chunks)
        self.hid_width = min(256, shard)
        self.hid_subs = shard // self.hid_width
        self.hid_blocks = vocab * self.hid_subs
        self.slots = 2 if self.line == 4 else self.line + 1


def fused_kernel(
    plan,
    hidden_ref, teacher_ref, weight_ref,
    kl_ref, hid_ref, out_ref,
    weight, student, grad, gathered, features, pair_grad, incoming, outgoing, block,
    pair_out, pair_in, hid_out, hid_in, hid_far_out, hid_far_in, hid_sum,
    row_student, row_teacher, lane_stats, stats,
    load_sem, weight_sem, out_sem,
    gather_send, gather_recv, fy_send, fy_recv, fz_send, fz_recv, fx_send, fx_recv, fc_send, fc_recv,
    stat_send, stat_recv, y_send, y_recv, zo_send, zo_recv, zf_send, zf_recv,
    line_send, line_recv, last_send, last_recv,
    hc_send, hc_recv, hx_send, hx_recv,
):
    line, vocab, chips = plan.line, plan.vocab, plan.chips
    tokens, shard, half, width, chunks = plan.tokens, plan.shard, plan.half, plan.width, plan.chunks
    rows2, rows, half_tokens = plan.rows2, plan.rows, plan.half_tokens
    columns = plan.columns

    me = lax.axis_index("dp")
    v = lax.axis_index("vocab")
    place = me // PAIR
    side = me - place * PAIR
    partner = place * PAIR + (PAIR - 1) - side
    chip = v // CORES
    core = v - chip * CORES
    other_core = chip * CORES + (CORES - 1) - core
    has_down = place > 0
    has_up = place < line - 1
    up = jnp.where(has_up, me + PAIR, me)
    down = jnp.where(has_down, me - PAIR, me)
    is_low = place == 0
    is_high = place == line - 1
    is_end = jnp.logical_or(is_low, is_high)
    next_low = place == 1
    next_high = place == line - 2
    is_next = jnp.logical_or(next_low, next_high)
    inner = jnp.where(is_low, up, down)

    def chip_after(step):
        return lax.rem(chip + step, chips)

    def chip_before(step):
        return lax.rem(chip + chips - step, chips)

    def shard_of(index):
        return pl.ds(pl.multiple_of(index * shard, shard), shard)

    def chip_rows(index):
        return pl.ds(pl.multiple_of(index * CORES * shard, CORES * shard), CORES * shard)

    def token_half(part):
        return pl.ds(part * half_tokens, half_tokens)

    def columns_of(chunk):
        return pl.ds(pl.multiple_of(chunk * width, width), width)

    def grad_columns(which, chunk):
        return pl.ds(pl.multiple_of(which * half + chunk * width, width), width)

    def remote(src, dst, send, recv, **target):
        return pltpu.make_async_remote_copy(
            src_ref=src, dst_ref=dst, send_sem=send, recv_sem=recv, device_id=target, device_id_type=MESH
        )

    own_load = pltpu.make_async_copy(hidden_ref, gathered.at[:, shard_of(v)], load_sem.at[0])
    teacher_load = pltpu.make_async_copy(teacher_ref, grad, load_sem.at[1])

    dot_width = plan.dot_width
    dot_blocks = columns // dot_width

    def dot_columns(index):
        return pl.ds(pl.multiple_of(index * dot_width, dot_width), dot_width)

    def weight_load(step, index):
        spot = (chip_rows(chip_before(step)), dot_columns(index))
        return pltpu.make_async_copy(weight_ref.at[spot], weight.at[spot], weight_sem.at[step, index])

    def load_weights(step):
        @pl.loop(0, dot_blocks)
        def _(index):
            weight_load(step, index).start()

    barrier = pltpu.get_barrier_semaphore()
    for step in range(1, vocab):
        pl.semaphore_signal(
            barrier, inc=1, device_id={"vocab": lax.rem(v + step, vocab)}, device_id_type=MESH
        )
    pl.semaphore_signal(barrier, inc=1, device_id={"dp": partner}, device_id_type=MESH)

    @pl.when(has_down)
    def _():
        pl.semaphore_signal(barrier, inc=1, device_id={"dp": down}, device_id_type=MESH)

    @pl.when(has_up)
    def _():
        pl.semaphore_signal(barrier, inc=1, device_id={"dp": up}, device_id_type=MESH)

    own_load.start()
    load_weights(0)
    teacher_load.start()
    for step in range(1, chips):
        load_weights(step)
    own_load.wait()
    pl.semaphore_wait(barrier, vocab + has_down.astype(jnp.int32) + has_up.astype(jnp.int32))

    def gather_copy(index, part, column, target):
        ref = gathered.at[token_half(part), shard_of(column)]
        return remote(ref, ref, gather_send.at[index, part], gather_recv.at[index, part], vocab=target)

    def gather_far(step, part):
        return gather_copy(step, part, v, chip_after(step) * CORES + core)

    def gather_pass(step, part):
        return gather_copy(chips - 1 + step, part, chip_before(step) * CORES + core, other_core)

    for part in range(plan.halves):
        for step in range(1, chips):
            gather_far(step, part).start()
        gather_copy(0, part, v, other_core).start()

    def set_ref(which, index, part):
        return features.at[shard_of(index), pl.ds(which * tokens + part * half_tokens, half_tokens)]

    def turn(index, part):
        features[shard_of(index), part * half_tokens : (part + 1) * half_tokens] = gathered[
            token_half(part), shard_of(index)
        ].T

    def feature_y(step, part):
        index = chip_before(step) * CORES + core
        return remote(
            set_ref(0, index, part), set_ref(1, index, part), fy_send.at[step, part], fy_recv.at[step, part],
            dp=partner,
        )

    def feature_z(which, part):
        return remote(
            set_ref(which, v, part), set_ref(2 + which, v, part), fz_send.at[which, part], fz_recv.at[which, part],
            dp=inner,
        )

    def feature_x(which, step, part):
        ref = set_ref(which, v, part)
        return remote(
            ref, ref, fx_send.at[which - 2, step, part], fx_recv.at[which - 2, step, part],
            vocab=chip_after(step) * CORES + core,
        )

    def feature_core(which, step, part):
        ref = set_ref(which, chip_before(step) * CORES + core, part)
        return remote(
            ref, ref, fc_send.at[which - 1, step, part], fc_recv.at[which - 1, step, part], vocab=other_core
        )

    for part in range(plan.halves):
        turn(v, part)
        feature_y(0, part).start()

        @pl.when(is_end)
        def _():
            feature_z(0, part).start()

    for part in range(plan.halves):
        gather_copy(0, part, other_core, other_core).wait_recv()

    def local_logits():
        @pl.loop(0, dot_blocks)
        def _(index):
            where = dot_columns(index)
            weight_load(0, index).wait()
            student[:, where] = jnp.dot(
                gathered[:, chip_rows(chip)], weight[chip_rows(chip), where], preferred_element_type=f32
            )

    band = 32

    def teacher_tops():
        @pl.loop(0, tokens // band)
        def _(index):
            where = pl.ds(pl.multiple_of(index * band, band), band)
            top = grad[where, 0:LANES]
            for column in range(1, columns // LANES):
                top = jnp.maximum(top, grad[where, column * LANES : (column + 1) * LANES])
            lane_stats[0, where, :] = top.astype(f32)

        row_teacher[...] = jnp.broadcast_to(jnp.max(lane_stats[0], axis=1, keepdims=True), (tokens, LANES))

    local_logits()
    teacher_load.wait()
    teacher_tops()
    for part in range(plan.halves):
        turn(other_core, part)

    def stat_copy(step, part, owner, target):
        ref = stats.at[owner, :, token_half(part)]
        return remote(ref, ref, stat_send.at[step, part], stat_recv.at[step, part], vocab=target)

    def await_far(part):
        for step in range(1, chips):
            gather_copy(
                chips - 1 + step, part, chip_before(step) * CORES + (CORES - 1) - core, other_core
            ).wait_recv()

    def far_logits():
        lane_stats[0] = jnp.full((tokens, LANES), -jnp.inf, f32)

        @pl.loop(0, dot_blocks)
        def _(index):
            where = dot_columns(index)
            total = student[:, where]
            for step in range(1, chips):
                far = chip_rows(chip_before(step))
                weight_load(step, index).wait()
                total = total + jnp.dot(gathered[:, far], weight[far, where], preferred_element_type=f32)
            student[:, where] = total
            top = lane_stats[0]
            for column in range(dot_width // LANES):
                top = jnp.maximum(top, total[:, column * LANES : (column + 1) * LANES])
            lane_stats[0] = top

    def student_tops(part):
        where_rows = token_half(part)
        student_top = jnp.max(lane_stats[0, where_rows, :], axis=1, keepdims=True)
        row_student[where_rows, :] = jnp.broadcast_to(student_top, (half_tokens, LANES))

    def row_sums(part):
        @pl.loop(0, half_tokens // band)
        def _(index):
            where = pl.ds(pl.multiple_of(part * half_tokens + index * band, band), band)
            student_max, teacher_max = row_student[where, :], row_teacher[where, :]
            sums = [jnp.zeros((band, LANES), f32) for _ in range(3)]
            for column in range(columns // LANES):
                lanes = slice(column * LANES, (column + 1) * LANES)
                logit, target = student[where, lanes], grad[where, lanes].astype(f32)
                term = jnp.exp(target - teacher_max)
                student_term = jnp.exp(logit - student_max)
                student[where, lanes] = student_term
                sums[0] += student_term
                sums[1] += term
                sums[2] += term * (target - logit)
            for which in range(3):
                lane_stats[which, where, :] = sums[which]

    def send_stats(part):
        where_rows = token_half(part)
        lane = lax.broadcasted_iota(jnp.int32, (half_tokens, LANES), 1)
        packed = jnp.where(lane == 0, row_student[where_rows, :], row_teacher[where_rows, :])
        for which in range(3):
            total = jnp.sum(lane_stats[which, where_rows, :], axis=1, keepdims=True)
            packed = jnp.where(lane == 2 + which, jnp.broadcast_to(total, packed.shape), packed)
        stats[v, :, where_rows] = packed.T[0:8, :]
        for step in range(1, vocab):
            stat_copy(step, part, v, lax.rem(v + step, vocab)).start()

    def pass_on(part):
        for step in range(1, chips):
            gather_copy(step, part, chip_before(step) * CORES + core, other_core).wait_recv()
            gather_pass(step, part).start()

    def y_copy(part, chunk):
        return remote(
            grad.at[token_half(part), grad_columns(PAIR - 1 - side, chunk)],
            pair_grad.at[token_half(part), columns_of(chunk)],
            y_send.at[part, chunk], y_recv.at[part, chunk], dp=partner,
        )

    def end_own(part, chunk):
        return remote(
            grad.at[token_half(part), grad_columns(side, chunk)],
            pair_grad.at[pl.ds(tokens + part * half_tokens, half_tokens), columns_of(chunk)],
            zo_send.at[part, chunk], zo_recv.at[part, chunk], dp=inner,
        )

    def end_pair(part, chunk):
        return remote(
            pair_grad.at[token_half(part), columns_of(chunk)],
            pair_grad.at[pl.ds(2 * tokens + part * half_tokens, half_tokens), columns_of(chunk)],
            zf_send.at[part, chunk], zf_recv.at[part, chunk], dp=inner,
        )

    def combine(part):
        where_rows = token_half(part)
        for step in range(1, vocab):
            stat_copy(step, part, lax.rem(v + vocab - step, vocab), other_core).wait_recv()
        parts = [stats[index, :, where_rows] for index in range(vocab)]
        student_max = functools.reduce(jnp.maximum, [p[0:1] for p in parts])
        teacher_max = functools.reduce(jnp.maximum, [p[1:2] for p in parts])
        student_total = sum(p[2:3] * jnp.exp(p[0:1] - student_max) for p in parts)
        teacher_scales = [jnp.exp(p[1:2] - teacher_max) for p in parts]
        teacher_total = sum(p[3:4] * scale for p, scale in zip(parts, teacher_scales))
        cross = sum(p[4:5] * scale for p, scale in zip(parts, teacher_scales))
        student_log = student_max + jnp.log(student_total)
        teacher_log = teacher_max + jnp.log(teacher_total)
        kl_ref[:, where_rows] = cross / teacher_total - teacher_log + student_log
        student_scale = grad_scale * jnp.exp(stats[v, 0:1, where_rows] - student_log)
        row = lax.broadcasted_iota(jnp.int32, (LANES, half_tokens), 0)
        packed = jnp.where(
            row == 0,
            jnp.broadcast_to(student_scale, (LANES, half_tokens)),
            jnp.broadcast_to(teacher_log - math.log(grad_scale), (LANES, half_tokens)),
        ).T
        row_student[where_rows, :] = jnp.broadcast_to(packed[:, 0:1], (half_tokens, LANES))
        row_teacher[where_rows, :] = jnp.broadcast_to(packed[:, 1:2], (half_tokens, LANES))

    def grads(part):
        @pl.loop(0, half_tokens // band)
        def _(index):
            where = pl.ds(pl.multiple_of(part * half_tokens + index * band, band), band)
            student_row, teacher_row = row_student[where, :], row_teacher[where, :]
            for column in range(columns // LANES):
                lanes = slice(column * LANES, (column + 1) * LANES)
                value = student[where, lanes] * student_row - jnp.exp(
                    grad[where, lanes].astype(f32) - teacher_row
                )
                grad[where, lanes] = value.astype(bf16)

    def send_grads(part):
        @pl.loop(0, plan.first)
        def _(chunk):
            y_copy(part, chunk).start()

        @pl.when(is_end)
        def _():
            for chunk in range(plan.ahead):
                end_own(part, chunk).start()

        if part == plan.halves - 1:

            @pl.loop(plan.first, chunks)
            def _(chunk):
                for each in range(plan.halves):
                    y_copy(each, chunk).start()

    def first_service(part):
        feature_y(0, part).wait_recv()
        feature_core(1, 0, part).start()

        @pl.when(is_end)
        def _():
            feature_z(1, part).start()

        @pl.when(is_next)
        def _():
            feature_z(0, part).wait_recv()
            for step in range(1, chips):
                feature_x(2, step, part).start()
            feature_core(2, 0, part).start()

    def turn_far(part):
        for step in range(1, chips):
            turn(chip_before(step) * CORES + core, part)
            feature_y(step, part).start()
        for step in range(1, chips):
            turn(chip_before(step) * CORES + (CORES - 1) - core, part)

    def middle_service(part):
        @pl.when(is_next)
        def _():
            feature_z(1, part).wait_recv()
            for step in range(1, chips):
                feature_x(3, step, part).start()
            feature_core(3, 0, part).start()
            for step in range(1, chips):
                feature_x(2, step, part).wait_recv()
                feature_core(2, step, part).start()

    def second_service(part):
        for step in range(1, chips):
            feature_y(step, part).wait_recv()
            feature_core(1, step, part).start()

    def last_service(part):
        @pl.when(is_next)
        def _():
            for step in range(1, chips):
                feature_x(3, step, part).wait_recv()
                feature_core(3, step, part).start()

    def await_features(part):
        for step in range(chips):
            feature_core(1, step, part).wait_recv()

        @pl.when(is_next)
        def _():
            for which in (2, 3):
                for step in range(chips):
                    feature_core(which, step, part).wait_recv()

    every = range(plan.halves)
    for part in every:
        pass_on(part)
        first_service(part)
        await_far(part)
        turn_far(part)
    far_logits()
    for part in every:
        student_tops(part)
        row_sums(part)
        send_stats(part)
    for part in every:
        middle_service(part)
    for part in every:
        combine(part)
        grads(part)
        send_grads(part)
    for service in (second_service, last_service, await_features):
        for part in every:
            service(part)

    def hid_core(index):
        return remote(
            hid_out.at[index], hid_in.at[index], hc_send.at[index], hc_recv.at[index], vocab=other_core
        )

    def hid_far(index):
        return remote(
            hid_far_out.at[index], hid_far_in.at[index], hx_send.at[index], hx_recv.at[index],
            vocab=lax.rem(chip + 1 + index, chips) * CORES + core,
        )

    def hid_block(index):
        piece = index // plan.hid_subs
        sub = index - piece * plan.hid_subs
        mine = piece >= chips
        order = jnp.where(mine, piece - chips, piece)
        target = lax.rem(chip + 1 + order, chips) * CORES + jnp.where(mine, core, (CORES - 1) - core)
        where = pl.ds(pl.multiple_of(target * shard + sub * plan.hid_width, plan.hid_width), plan.hid_width)
        lanes = pl.ds(pl.multiple_of(sub * plan.hid_width, plan.hid_width), plan.hid_width)
        last_sub = sub == plan.hid_subs - 1
        value = lax.dot_general(
            grad[...], weight[where, :], (((1,), (1,)), ((), ())), preferred_element_type=f32
        )

        @pl.when(jnp.logical_not(mine))
        def _():
            hid_out[order, :, lanes] = value.astype(bf16)

            @pl.when(last_sub)
            def _():
                hid_core(order).start()

        @pl.when(mine)
        def _():
            @pl.when(sub == 0)
            def _():
                hid_core(order).wait_recv()

            total = value + hid_in[order, :, lanes].astype(f32)

            @pl.when(order < chips - 1)
            def _():
                hid_far_out[order, :, lanes] = total.astype(bf16)

                @pl.when(last_sub)
                def _():
                    hid_far(order).start()

            @pl.when(order == chips - 1)
            def _():
                hid_sum[:, lanes] = total

    def hid_finish():
        total = hid_sum[...]
        for index in range(chips - 1):
            hid_far(index).wait_recv()
            total = total + hid_far_in[index].astype(f32)
        hid_ref[...] = total.astype(bf16)
        for step in range(chips):
            hid_core(step).wait_send()
        for index in range(chips - 1):
            hid_far(index).wait_send()

    def rows_of(part):
        return pl.ds(pl.multiple_of(part * rows2, rows2), rows2)

    def sum_into_block(part, chunk, with_end):
        where = columns_of(chunk)
        block[...] = jnp.dot(
            features[rows_of(part), 0:tokens], grad[:, grad_columns(side, chunk)], preferred_element_type=f32
        ) + jnp.dot(
            features[rows_of(part), tokens : 2 * tokens], pair_grad[0:tokens, where], preferred_element_type=f32
        )

        def add_end():
            block[...] += jnp.dot(
                features[rows_of(part), 2 * tokens : 4 * tokens],
                pair_grad[tokens : 3 * tokens, where],
                preferred_element_type=f32,
            )

        if with_end is True:
            add_end()
        elif with_end is not False:
            pl.when(with_end)(add_end)

    def base_slot(where):
        return jnp.where(jnp.logical_and(where >= 1, where <= line - 3), where + 1, 0)

    def line_copy(chunk, part, slot, target):
        return remote(
            outgoing.at[lax.rem(chunk, plan.window), part],
            incoming.at[slot, :, columns_of(chunk)],
            line_send.at[part, chunk], line_recv.at[slot, chunk], dp=target,
        )

    def send_sum(chunk, part, target, slot, source):
        @pl.when(chunk >= plan.window)
        def _():
            line_copy(chunk - plan.window, part, slot, target).wait_send()

        spot = lax.rem(chunk, plan.window)
        if source is None:
            outgoing[spot, part] = block[...].astype(bf16)
        else:
            has_source, source_slot = source

            @pl.when(has_source)
            def _():
                line_copy(chunk, part, source_slot, target).wait_recv()
                outgoing[spot, part] = (
                    block[...] + incoming[source_slot, :, columns_of(chunk)].astype(f32)
                ).astype(bf16)

            @pl.when(jnp.logical_not(has_source))
            def _():
                outgoing[spot, part] = block[...].astype(bf16)

        line_copy(chunk, part, slot, target).start()

    def up_slot(part):
        return base_slot(place + 1) + part - place - 1

    from_below = jnp.logical_and(place >= 2, jnp.logical_not(is_low))
    from_above = place <= line - 3

    def last_copy(chunk):
        return remote(
            pair_out.at[:, columns_of(chunk)], pair_in.at[:, columns_of(chunk)],
            last_send.at[chunk], last_recv.at[chunk], dp=partner,
        )

    def add_incoming(chunk, slot):
        line_copy(chunk, 0, slot, me).wait_recv()
        block[...] += incoming[slot, :, columns_of(chunk)].astype(f32)

    def settle(chunk):
        student[0:rows, grad_columns(side, chunk)] = block[
            pl.ds(pl.multiple_of(side * rows, rows), rows), :
        ]
        pair_out[:, columns_of(chunk)] = block[
            pl.ds(pl.multiple_of((PAIR - 1 - side) * rows, rows), rows), :
        ].astype(bf16)
        last_copy(chunk).start()

    def result_copy(which, chunk):
        spot = grad_columns(jnp.where(which == 0, side, PAIR - 1 - side), chunk)
        return pltpu.make_async_copy(student.at[0:rows, spot], out_ref.at[:, spot], out_sem.at[which, chunk])

    def early_sums(chunk):
        @pl.loop(0, line - 2)
        def _(index):
            part = jnp.where(next_low, line - 1 - index, index)
            sum_into_block(part, chunk, True)
            send_sum(
                chunk, part, jnp.where(next_low, up, down), jnp.where(next_low, up_slot(part), part), None
            )

    def late_sums(chunk):
        @pl.when(place >= 2)
        def _():
            @pl.loop(0, line - 1 - place)
            def _(index):
                part = line - 1 - index
                sum_into_block(part, chunk, False)
                send_sum(chunk, part, up, up_slot(part), (from_below, base_slot(place) + part - place))

        @pl.when(place <= line - 3)
        def _():
            @pl.loop(0, place)
            def _(part):
                sum_into_block(part, chunk, False)
                send_sum(chunk, part, down, part, (from_above, part))

        sum_into_block(place, chunk, is_next)

        @pl.when(from_below)
        def _():
            add_incoming(chunk, base_slot(place))

        @pl.when(from_above)
        def _():
            add_incoming(chunk, place)

        settle(chunk)

    def drain():
        for part in every:
            for step in range(1, chips):
                gather_far(step, part).wait_send()
                gather_pass(step, part).wait_send()
            gather_copy(0, part, v, other_core).wait_send()
            for step in range(1, vocab):
                stat_copy(step, part, v, lax.rem(v + step, vocab)).wait_send()
            for step in range(chips):
                feature_y(step, part).wait_send()
                feature_core(1, step, part).wait_send()

            @pl.when(is_end)
            def _():
                for which in range(2):
                    feature_z(which, part).wait_send()

            @pl.when(is_next)
            def _():
                for which in (2, 3):
                    feature_core(which, 0, part).wait_send()
                    for step in range(1, chips):
                        feature_x(which, step, part).wait_send()
                        feature_core(which, step, part).wait_send()

        @pl.loop(0, chunks)
        def _(chunk):
            for part in every:
                y_copy(part, chunk).wait_send()

        @pl.when(is_end)
        def _():
            @pl.loop(0, chunks)
            def _(chunk):
                for part in every:
                    end_own(part, chunk).wait_send()
                    end_pair(part, chunk).wait_send()

    @pl.loop(0, chunks + plan.last_lag)
    def _(step):
        @pl.when(step < plan.hid_blocks)
        def _():
            hid_block(step)

        if plan.hid_blocks < chunks + plan.last_lag:
            pl.when(step == max(plan.hid_blocks, chunks))(hid_finish)

        pl.when(step == chunks + plan.lag - 1)(drain)

        @pl.when(step < chunks)
        def _():
            for part in range(plan.halves):
                y_copy(part, step).wait_recv()

            @pl.when(is_end)
            def _():
                for part in range(plan.halves):
                    end_pair(part, step).start()

                @pl.when(step + plan.ahead < chunks)
                def _():
                    for part in range(plan.halves):
                        end_own(part, step + plan.ahead).start()

            @pl.when(is_next)
            def _():
                for part in range(plan.halves):
                    end_own(part, step).wait_recv()
                    end_pair(part, step).wait_recv()
                early_sums(step)

        @pl.when(
            jnp.logical_and(
                jnp.logical_not(is_end),
                jnp.logical_and(step >= plan.lag, step < chunks + plan.lag),
            )
        )
        def _():
            late_sums(step - plan.lag)

        @pl.when(
            jnp.logical_and(is_end, jnp.logical_and(step >= plan.end_lag, step < chunks + plan.end_lag))
        )
        def _():
            chunk = step - plan.end_lag
            sum_into_block(place, chunk, False)
            add_incoming(chunk, 0)
            settle(chunk)

        @pl.when(step >= plan.last_lag)
        def _():
            chunk = step - plan.last_lag
            last_copy(chunk).wait_recv()
            student[0:rows, grad_columns(PAIR - 1 - side, chunk)] = pair_in[:, columns_of(chunk)].astype(f32)
            result_copy(0, chunk).start()
            result_copy(1, chunk).start()

    @pl.loop(min(chunks + plan.last_lag, plan.hid_blocks), plan.hid_blocks)
    def _(index):
        hid_block(index)

    if plan.hid_blocks >= chunks + plan.last_lag:
        hid_finish()

    @pl.loop(0, chunks)
    def _(chunk):
        last_copy(chunk).wait_send()
        result_copy(0, chunk).wait()
        result_copy(1, chunk).wait()

    @pl.when(jnp.logical_not(is_end))
    def _():
        @pl.loop(chunks - plan.window, chunks)
        def _(chunk):
            @pl.loop(0, place)
            def _(part):
                line_copy(chunk, part, 0, down).wait_send()

            @pl.loop(place + 1, line)
            def _(part):
                line_copy(chunk, part, 0, up).wait_send()


def per_device(shards, vocab, hidden_states, teacher_logits, head_weight):
    tokens, shard = hidden_states.shape
    model_width, columns = head_weight.shape
    plan = Plan(shards, vocab, tokens, shard, model_width, columns)
    dma = pltpu.SemaphoreType.DMA
    chips, halves, chunks = plan.chips, plan.halves, plan.chunks
    any_space = pl.BlockSpec(memory_space=pl.ANY)
    in_vmem = pl.BlockSpec(memory_space=pltpu.VMEM)
    divergence, hidden_grad, head_grad = pl.pallas_call(
        functools.partial(fused_kernel, plan),
        out_shape=(
            jax.ShapeDtypeStruct((1, tokens), f32),
            jax.ShapeDtypeStruct((tokens, shard), bf16),
            jax.ShapeDtypeStruct((plan.rows, columns), f32),
        ),
        in_specs=[any_space] * 3,
        out_specs=(in_vmem, in_vmem, any_space),
        scratch_shapes=[
            pltpu.VMEM((model_width, columns), bf16),
            pltpu.VMEM((tokens, columns), f32),
            pltpu.VMEM((tokens, columns), bf16),
            pltpu.VMEM((tokens, model_width), bf16),
            pltpu.VMEM((model_width, 4 * tokens), bf16),
            pltpu.VMEM((3 * tokens, plan.half), bf16),
            pltpu.VMEM((plan.slots, plan.rows2, plan.half), bf16),
            pltpu.VMEM((plan.window, plan.line, plan.rows2, plan.width), bf16),
            pltpu.VMEM((plan.rows2, plan.width), f32),
            pltpu.VMEM((plan.rows, plan.half), bf16),
            pltpu.VMEM((plan.rows, plan.half), bf16),
            pltpu.VMEM((chips, tokens, shard), bf16),
            pltpu.VMEM((chips, tokens, shard), bf16),
            pltpu.VMEM((chips - 1, tokens, shard), bf16),
            pltpu.VMEM((chips - 1, tokens, shard), bf16),
            pltpu.VMEM((tokens, shard), f32),
            pltpu.VMEM((tokens, LANES), f32),
            pltpu.VMEM((tokens, LANES), f32),
            pltpu.VMEM((3, tokens, LANES), f32),
            pltpu.VMEM((vocab, 8, tokens), f32),
            dma((2,)), dma((chips, columns // plan.dot_width)), dma((2, chunks)),
            dma((2 * chips - 1, halves)), dma((2 * chips - 1, halves)),
            dma((chips, halves)), dma((chips, halves)),
            dma((2, halves)), dma((2, halves)),
            dma((2, chips, halves)), dma((2, chips, halves)),
            dma((3, chips, halves)), dma((3, chips, halves)),
            dma((vocab, halves)), dma((vocab, halves)),
            dma((halves, chunks)), dma((halves, chunks)),
            dma((halves, chunks)), dma((halves, chunks)),
            dma((halves, chunks)), dma((halves, chunks)),
            dma((plan.line, chunks)), dma((plan.slots, chunks)),
            dma((chunks,)), dma((chunks,)),
            dma((chips,)), dma((chips,)),
            dma((chips - 1,)), dma((chips - 1,)),
        ],
        compiler_params=pltpu.CompilerParams(
            collective_id=0, has_side_effects=True, vmem_limit_bytes=67043328
        ),
    )(hidden_states, teacher_logits, head_weight)
    return divergence.reshape(tokens), hidden_grad, head_grad


def solution(mesh):
    in_specs = (P("dp", "vocab"), P("dp", "vocab"), P(None, "vocab"))
    out_specs = (P("dp"), P("dp", "vocab"), P("dp", "vocab"))
    return jax.shard_map(
        functools.partial(per_device, mesh.shape["dp"], mesh.shape["vocab"]),
        mesh=mesh, in_specs=in_specs, out_specs=out_specs, check_vma=False,
    )
```

```python
import functools
import math

import jax
import jax.numpy as jnp
from jax import lax
from jax.experimental import pallas as pl
from jax.experimental.pallas import tpu as pltpu
from jax.sharding import PartitionSpec as P

grad_scale = 8.0
PAIR = 2
CORES = 2
LANES = 128
MESH = pl.DeviceIdType.MESH
f32 = jnp.float32
bf16 = jnp.bfloat16


class Plan:
    def __init__(self, shards, vocab, tokens, shard, model_width, columns):
        self.line = shards // PAIR
        self.vocab = vocab
        self.chips = vocab // CORES
        self.tokens = tokens
        self.shard = shard
        self.model_width = model_width
        self.columns = columns
        self.halves = 2
        self.half_tokens = tokens // self.halves
        self.half_shard = shard // self.halves
        self.half = columns // PAIR
        self.width = min(128, self.half)
        self.chunks = self.half // self.width
        self.rows2 = model_width // self.line
        self.rows = self.rows2 // PAIR
        self.window = min(6, self.chunks)
        self.dot_width = min(512, columns)
        self.lag = 2
        self.end_lag = self.lag + 2
        self.last_lag = max(self.end_lag + 1, self.chunks // 2 + 2)
        self.ahead = 2
        self.first = 2
        self.hid_width = min(256, shard)
        self.hid_subs = shard // self.hid_width
        self.hid_blocks = vocab * self.hid_subs
        self.slots = 2 if self.line == 4 else self.line + 1


def fused_kernel(
    plan,
    hidden_ref, teacher_ref, weight_ref,
    kl_any, hid_any, own_any, pair_any,
    kl_ref, hid_ref, weight, student, grad, gathered, features, pair_grad, incoming, outgoing, block,
    pair_out, pair_in, hid_out, hid_in, hid_far_out, hid_far_in, hid_sum,
    row_student, row_teacher, lane_stats, stats,
    load_sem, weight_sem, out_sem,
    gather_send, gather_recv, fy_send, fy_recv, fz_send, fz_recv, fzf_send, fzf_recv, fx_send, fx_recv, fc_send, fc_recv,
    stat_send, stat_recv, y_send, y_recv, zo_send, zo_recv, zf_send, zf_recv,
    line_send, line_recv, last_send, last_recv,
    hc_send, hc_recv, hx_send, hx_recv,
):
    line, vocab, chips = plan.line, plan.vocab, plan.chips
    tokens, shard, half, width, chunks = plan.tokens, plan.shard, plan.half, plan.width, plan.chunks
    rows2, rows, half_tokens = plan.rows2, plan.rows, plan.half_tokens
    columns = plan.columns

    me = lax.axis_index("dp")
    v = lax.axis_index("vocab")
    place = me // PAIR
    side = me - place * PAIR
    partner = place * PAIR + (PAIR - 1) - side
    chip = v // CORES
    core = v - chip * CORES
    other_core = chip * CORES + (CORES - 1) - core
    has_down = place > 0
    has_up = place < line - 1
    up = jnp.where(has_up, me + PAIR, me)
    down = jnp.where(has_down, me - PAIR, me)
    is_low = place == 0
    is_high = place == line - 1
    is_end = jnp.logical_or(is_low, is_high)
    next_low = place == 1
    next_high = place == line - 2
    is_next = jnp.logical_or(next_low, next_high)
    inner = jnp.where(is_low, up, down)

    def chip_after(step):
        return lax.rem(chip + step, chips)

    def chip_before(step):
        return lax.rem(chip + chips - step, chips)

    def shard_of(index):
        return pl.ds(pl.multiple_of(index * shard, shard), shard)

    def chip_rows(index):
        return pl.ds(pl.multiple_of(index * CORES * shard, CORES * shard), CORES * shard)

    def token_half(part):
        return pl.ds(part * half_tokens, half_tokens)

    def columns_of(chunk):
        return pl.ds(pl.multiple_of(chunk * width, width), width)

    def grad_columns(which, chunk):
        return pl.ds(pl.multiple_of(which * half + chunk * width, width), width)

    def remote(src, dst, send, recv, **target):
        return pltpu.make_async_remote_copy(
            src_ref=src, dst_ref=dst, send_sem=send, recv_sem=recv, device_id=target, device_id_type=MESH
        )

    own_load = pltpu.make_async_copy(hidden_ref, gathered.at[:, shard_of(v)], load_sem.at[0])
    teacher_load = pltpu.make_async_copy(teacher_ref, grad, load_sem.at[1])

    dot_width = plan.dot_width
    dot_blocks = columns // dot_width

    def dot_columns(index):
        return pl.ds(pl.multiple_of(index * dot_width, dot_width), dot_width)

    def weight_load(step, index):
        spot = (chip_rows(chip_before(step)), dot_columns(index))
        return pltpu.make_async_copy(weight_ref.at[spot], weight.at[spot], weight_sem.at[step, index])

    def load_weights(step):
        @pl.loop(0, dot_blocks)
        def _(index):
            weight_load(step, index).start()

    barrier = pltpu.get_barrier_semaphore()
    for step in range(1, vocab):
        pl.semaphore_signal(
            barrier, inc=1, device_id={"vocab": lax.rem(v + step, vocab)}, device_id_type=MESH
        )
    pl.semaphore_signal(barrier, inc=1, device_id={"dp": partner}, device_id_type=MESH)

    @pl.when(has_down)
    def _():
        pl.semaphore_signal(barrier, inc=1, device_id={"dp": down}, device_id_type=MESH)

    @pl.when(has_up)
    def _():
        pl.semaphore_signal(barrier, inc=1, device_id={"dp": up}, device_id_type=MESH)

    own_load.start()
    load_weights(0)
    teacher_load.start()
    for step in range(1, chips):
        load_weights(step)
    own_load.wait()
    pl.semaphore_wait(barrier, vocab + has_down.astype(jnp.int32) + has_up.astype(jnp.int32))

    half_shard = plan.half_shard

    def shard_half(index, part):
        return pl.ds(pl.multiple_of(index * shard + part * half_shard, half_shard), half_shard)

    def gather_copy(index, part, column, target):
        ref = gathered.at[:, shard_half(column, part)]
        return remote(ref, ref, gather_send.at[index, part], gather_recv.at[index, part], vocab=target)

    def gather_far(step, part):
        return gather_copy(step, part, v, chip_after(step) * CORES + core)

    def gather_pass(step, part):
        return gather_copy(chips - 1 + step, part, chip_before(step) * CORES + core, other_core)

    for part in range(plan.halves):
        for step in range(1, chips):
            gather_far(step, part).start()
        gather_copy(0, part, v, other_core).start()

    def set_ref(which, index, part):
        return features.at[shard_half(index, part), pl.ds(which * tokens, tokens)]

    def turn(index, part):
        features[shard_half(index, part), 0:tokens] = gathered[:, shard_half(index, part)].T

    def feature_y(step, part):
        index = chip_before(step) * CORES + core
        return remote(
            set_ref(0, index, part), set_ref(1, index, part), fy_send.at[step, part], fy_recv.at[step, part],
            dp=partner,
        )

    def feature_z(which, part):
        return remote(
            set_ref(which, v, part), set_ref(2 + which, v, part), fz_send.at[which, part], fz_recv.at[which, part],
            dp=inner,
        )

    def feature_z_far(step):
        index = chip_before(step) * CORES + core
        return remote(set_ref(1, index, 0), set_ref(3, index, 0), fzf_send.at[step], fzf_recv.at[step], dp=inner)

    def feature_x(which, step, part):
        ref = set_ref(which, v, part)
        return remote(
            ref, ref, fx_send.at[which - 2, step, part], fx_recv.at[which - 2, step, part],
            vocab=chip_after(step) * CORES + core,
        )

    def feature_core(which, step, part):
        ref = set_ref(which, chip_before(step) * CORES + core, part)
        return remote(
            ref, ref, fc_send.at[which - 1, step, part], fc_recv.at[which - 1, step, part], vocab=other_core
        )

    for part in range(plan.halves):
        turn(v, part)
        feature_y(0, part).start()

        @pl.when(is_end)
        def _():
            feature_z(0, part).start()

    for part in range(plan.halves):
        gather_copy(0, part, other_core, other_core).wait_recv()

    def local_logits():
        @pl.loop(0, dot_blocks)
        def _(index):
            where = dot_columns(index)
            weight_load(0, index).wait()
            student[:, where] = jnp.dot(
                gathered[:, chip_rows(chip)], weight[chip_rows(chip), where], preferred_element_type=f32
            )

    band = 32

    def teacher_tops():
        @pl.loop(0, tokens // band)
        def _(index):
            where = pl.ds(pl.multiple_of(index * band, band), band)
            top = grad[where, 0:LANES]
            for column in range(1, columns // LANES):
                top = jnp.maximum(top, grad[where, column * LANES : (column + 1) * LANES])
            lane_stats[0, where, :] = top.astype(f32)

        row_teacher[...] = jnp.broadcast_to(jnp.max(lane_stats[0], axis=1, keepdims=True), (tokens, LANES))

    local_logits()
    teacher_load.wait()
    teacher_tops()
    for part in range(plan.halves):
        turn(other_core, part)

    def stat_copy(step, part, owner, target):
        ref = stats.at[owner, :, token_half(part)]
        return remote(ref, ref, stat_send.at[step, part], stat_recv.at[step, part], vocab=target)

    def await_far(part):
        for step in range(1, chips):
            gather_copy(
                chips - 1 + step, part, chip_before(step) * CORES + (CORES - 1) - core, other_core
            ).wait_recv()

    def far_logits(part):
        last = part == plan.halves - 1
        if last:
            lane_stats[0] = jnp.full((tokens, LANES), -jnp.inf, f32)

        @pl.loop(0, dot_blocks)
        def _(index):
            where = dot_columns(index)
            total = student[:, where]
            for step in range(1, chips):
                far = [chip_before(step) * CORES + each for each in range(CORES)]
                if part == 0:
                    weight_load(step, index).wait()
                total = total + jnp.dot(
                    jnp.concatenate([gathered[:, shard_half(each, part)] for each in far], axis=1),
                    jnp.concatenate([weight[shard_half(each, part), where] for each in far], axis=0),
                    preferred_element_type=f32,
                )
            student[:, where] = total
            if last:
                top = lane_stats[0]
                for column in range(dot_width // LANES):
                    top = jnp.maximum(top, total[:, column * LANES : (column + 1) * LANES])
                lane_stats[0] = top

    def student_tops(part):
        where_rows = token_half(part)
        student_top = jnp.max(lane_stats[0, where_rows, :], axis=1, keepdims=True)
        row_student[where_rows, :] = jnp.broadcast_to(student_top, (half_tokens, LANES))

    def row_sums(part):
        @pl.loop(0, half_tokens // band)
        def _(index):
            where = pl.ds(pl.multiple_of(part * half_tokens + index * band, band), band)
            student_max, teacher_max = row_student[where, :], row_teacher[where, :]
            sums = [jnp.zeros((band, LANES), f32) for _ in range(3)]
            for column in range(columns // LANES):
                lanes = slice(column * LANES, (column + 1) * LANES)
                logit, target = student[where, lanes], grad[where, lanes].astype(f32)
                term = jnp.exp(target - teacher_max)
                student_term = jnp.exp(logit - student_max)
                student[where, lanes] = student_term
                sums[0] += student_term
                sums[1] += term
                sums[2] += term * (target - logit)
            for which in range(3):
                lane_stats[which, where, :] = sums[which]

    def send_stats(part):
        where_rows = token_half(part)
        lane = lax.broadcasted_iota(jnp.int32, (half_tokens, LANES), 1)
        packed = jnp.where(lane == 0, row_student[where_rows, :], row_teacher[where_rows, :])
        for which in range(3):
            total = jnp.sum(lane_stats[which, where_rows, :], axis=1, keepdims=True)
            packed = jnp.where(lane == 2 + which, jnp.broadcast_to(total, packed.shape), packed)
        stats[v, :, where_rows] = packed.T[0:8, :]
        for step in range(1, vocab):
            stat_copy(step, part, v, lax.rem(v + step, vocab)).start()

    def pass_on(part):
        for step in range(1, chips):
            gather_copy(step, part, chip_before(step) * CORES + core, other_core).wait_recv()
            gather_pass(step, part).start()

    def y_copy(part, chunk):
        return remote(
            grad.at[token_half(part), grad_columns(PAIR - 1 - side, chunk)],
            pair_grad.at[token_half(part), columns_of(chunk)],
            y_send.at[part, chunk], y_recv.at[part, chunk], dp=partner,
        )

    def end_own(part, chunk):
        return remote(
            grad.at[token_half(part), grad_columns(side, chunk)],
            pair_grad.at[pl.ds(tokens + part * half_tokens, half_tokens), columns_of(chunk)],
            zo_send.at[part, chunk], zo_recv.at[part, chunk], dp=inner,
        )

    def end_pair(part, chunk):
        return remote(
            pair_grad.at[token_half(part), columns_of(chunk)],
            pair_grad.at[pl.ds(2 * tokens + part * half_tokens, half_tokens), columns_of(chunk)],
            zf_send.at[part, chunk], zf_recv.at[part, chunk], dp=inner,
        )

    def combine(part):
        where_rows = token_half(part)
        for step in range(1, vocab):
            stat_copy(step, part, lax.rem(v + vocab - step, vocab), other_core).wait_recv()
        parts = [stats[index, :, where_rows] for index in range(vocab)]
        student_max = functools.reduce(jnp.maximum, [p[0:1] for p in parts])
        teacher_max = functools.reduce(jnp.maximum, [p[1:2] for p in parts])
        student_total = sum(p[2:3] * jnp.exp(p[0:1] - student_max) for p in parts)
        teacher_scales = [jnp.exp(p[1:2] - teacher_max) for p in parts]
        teacher_total = sum(p[3:4] * scale for p, scale in zip(parts, teacher_scales))
        cross = sum(p[4:5] * scale for p, scale in zip(parts, teacher_scales))
        student_log = student_max + jnp.log(student_total)
        teacher_log = teacher_max + jnp.log(teacher_total)
        kl_ref[:, where_rows] = cross / teacher_total - teacher_log + student_log
        student_scale = grad_scale * jnp.exp(stats[v, 0:1, where_rows] - student_log)
        row = lax.broadcasted_iota(jnp.int32, (LANES, half_tokens), 0)
        packed = jnp.where(
            row == 0,
            jnp.broadcast_to(student_scale, (LANES, half_tokens)),
            jnp.broadcast_to(teacher_log - math.log(grad_scale), (LANES, half_tokens)),
        ).T
        row_student[where_rows, :] = jnp.broadcast_to(packed[:, 0:1], (half_tokens, LANES))
        row_teacher[where_rows, :] = jnp.broadcast_to(packed[:, 1:2], (half_tokens, LANES))

    def grads(part):
        @pl.loop(0, half_tokens // band)
        def _(index):
            where = pl.ds(pl.multiple_of(part * half_tokens + index * band, band), band)
            student_row, teacher_row = row_student[where, :], row_teacher[where, :]
            for column in range(columns // LANES):
                lanes = slice(column * LANES, (column + 1) * LANES)
                value = student[where, lanes] * student_row - jnp.exp(
                    grad[where, lanes].astype(f32) - teacher_row
                )
                grad[where, lanes] = value.astype(bf16)

    def send_grads(part):
        @pl.loop(0, plan.first)
        def _(chunk):
            y_copy(part, chunk).start()

        @pl.when(is_end)
        def _():
            for chunk in range(plan.ahead):
                end_own(part, chunk).start()

        if part == plan.halves - 1:

            @pl.loop(plan.first, chunks)
            def _(chunk):
                for each in range(plan.halves):
                    y_copy(each, chunk).start()

    def first_service(part):
        feature_y(0, part).wait_recv()
        feature_core(1, 0, part).start()

        @pl.when(is_end)
        def _():
            feature_z(1, part).start()

        @pl.when(is_next)
        def _():
            feature_z(0, part).wait_recv()
            for step in range(1, chips):
                feature_x(2, step, part).start()
            feature_core(2, 0, part).start()

    def turn_far(part):
        for step in range(1, chips):
            turn(chip_before(step) * CORES + core, part)
            feature_y(step, part).start()
        for step in range(1, chips):
            turn(chip_before(step) * CORES + (CORES - 1) - core, part)

    def middle_service(part):
        @pl.when(is_next)
        def _():
            feature_z(1, part).wait_recv()
            if part > 0:
                for step in range(1, chips):
                    feature_x(3, step, part).start()
            feature_core(3, 0, part).start()
            for step in range(1, chips):
                feature_x(2, step, part).wait_recv()
                feature_core(2, step, part).start()

    def second_service(part):
        for step in range(1, chips):
            feature_y(step, part).wait_recv()
            feature_core(1, step, part).start()

            if part == 0:
                pl.when(is_end)(feature_z_far(step).start)

    def last_service(part):
        @pl.when(is_next)
        def _():
            for step in range(1, chips):
                if part > 0:
                    feature_x(3, step, part).wait_recv()
                else:
                    feature_z_far(step).wait_recv()
                feature_core(3, step, part).start()

    def await_features(part):
        for step in range(chips):
            feature_core(1, step, part).wait_recv()

        @pl.when(is_next)
        def _():
            for which in (2, 3):
                for step in range(chips):
                    feature_core(which, step, part).wait_recv()

    every = range(plan.halves)
    for part in every:
        pass_on(part)
        first_service(part)
        await_far(part)
        turn_far(part)
        far_logits(part)
    second_service(0)
    for part in every:
        student_tops(part)
        row_sums(part)
        send_stats(part)
    for part in every:
        middle_service(part)
    for part in every:
        combine(part)
        grads(part)
        send_grads(part)
    for part in every[1:]:
        second_service(part)
    for part in every:
        last_service(part)
    for part in every:
        await_features(part)

    def hid_core(index):
        return remote(
            hid_out.at[index], hid_in.at[index], hc_send.at[index], hc_recv.at[index], vocab=other_core
        )

    def hid_far(index):
        return remote(
            hid_far_out.at[index], hid_far_in.at[index], hx_send.at[index], hx_recv.at[index],
            vocab=lax.rem(chip + 1 + index, chips) * CORES + core,
        )

    def hid_block(index):
        piece = index // plan.hid_subs
        sub = index - piece * plan.hid_subs
        mine = piece >= chips
        order = jnp.where(mine, piece - chips, piece)
        target = lax.rem(chip + 1 + order, chips) * CORES + jnp.where(mine, core, (CORES - 1) - core)
        where = pl.ds(pl.multiple_of(target * shard + sub * plan.hid_width, plan.hid_width), plan.hid_width)
        lanes = pl.ds(pl.multiple_of(sub * plan.hid_width, plan.hid_width), plan.hid_width)
        last_sub = sub == plan.hid_subs - 1
        value = lax.dot_general(
            grad[...], weight[where, :], (((1,), (1,)), ((), ())), preferred_element_type=f32
        )

        @pl.when(jnp.logical_not(mine))
        def _():
            hid_out[order, :, lanes] = value.astype(bf16)

            @pl.when(last_sub)
            def _():
                hid_core(order).start()

        @pl.when(mine)
        def _():
            @pl.when(sub == 0)
            def _():
                hid_core(order).wait_recv()

            total = value + hid_in[order, :, lanes].astype(f32)

            @pl.when(order < chips - 1)
            def _():
                hid_far_out[order, :, lanes] = total.astype(bf16)

                @pl.when(last_sub)
                def _():
                    hid_far(order).start()

            @pl.when(order == chips - 1)
            def _():
                hid_sum[:, lanes] = total

    hid_store = pltpu.make_async_copy(hid_ref, hid_any, load_sem.at[2])
    kl_store = pltpu.make_async_copy(kl_ref, kl_any, load_sem.at[3])
    kl_store.start()

    def hid_finish():
        total = hid_sum[...]
        for index in range(chips - 1):
            hid_far(index).wait_recv()
            total = total + hid_far_in[index].astype(f32)
        hid_ref[...] = total.astype(bf16)
        hid_store.start()
        for step in range(chips):
            hid_core(step).wait_send()
        for index in range(chips - 1):
            hid_far(index).wait_send()

    def rows_of(part):
        return pl.ds(pl.multiple_of(part * rows2, rows2), rows2)

    def sum_into_block(part, chunk, with_end):
        where = columns_of(chunk)
        block[...] = jnp.dot(
            features[rows_of(part), 0:tokens], grad[:, grad_columns(side, chunk)], preferred_element_type=f32
        ) + jnp.dot(
            features[rows_of(part), tokens : 2 * tokens], pair_grad[0:tokens, where], preferred_element_type=f32
        )

        def add_end():
            block[...] += jnp.dot(
                features[rows_of(part), 2 * tokens : 4 * tokens],
                pair_grad[tokens : 3 * tokens, where],
                preferred_element_type=f32,
            )

        if with_end is True:
            add_end()
        elif with_end is not False:
            pl.when(with_end)(add_end)

    def base_slot(where):
        return jnp.where(jnp.logical_and(where >= 1, where <= line - 3), where + 1, 0)

    def line_copy(chunk, part, slot, target):
        return remote(
            outgoing.at[lax.rem(chunk, plan.window), part],
            incoming.at[slot, :, columns_of(chunk)],
            line_send.at[part, chunk], line_recv.at[slot, chunk], dp=target,
        )

    def send_sum(chunk, part, target, slot, source):
        @pl.when(chunk >= plan.window)
        def _():
            line_copy(chunk - plan.window, part, slot, target).wait_send()

        spot = lax.rem(chunk, plan.window)
        if source is None:
            outgoing[spot, part] = block[...].astype(bf16)
        else:
            has_source, source_slot = source

            @pl.when(has_source)
            def _():
                line_copy(chunk, part, source_slot, target).wait_recv()
                outgoing[spot, part] = (
                    block[...] + incoming[source_slot, :, columns_of(chunk)].astype(f32)
                ).astype(bf16)

            @pl.when(jnp.logical_not(has_source))
            def _():
                outgoing[spot, part] = block[...].astype(bf16)

        line_copy(chunk, part, slot, target).start()

    def up_slot(part):
        return base_slot(place + 1) + part - place - 1

    from_below = jnp.logical_and(place >= 2, jnp.logical_not(is_low))
    from_above = place <= line - 3

    def last_copy(chunk):
        return remote(
            pair_out.at[:, columns_of(chunk)], pair_in.at[:, columns_of(chunk)],
            last_send.at[chunk], last_recv.at[chunk], dp=partner,
        )

    def add_incoming(chunk, slot):
        line_copy(chunk, 0, slot, me).wait_recv()
        block[...] += incoming[slot, :, columns_of(chunk)].astype(f32)

    def settle(chunk):
        pair_out[:, columns_of(chunk)] = block[
            pl.ds(pl.multiple_of((PAIR - 1 - side) * rows, rows), rows), :
        ].astype(bf16)
        last_copy(chunk).start()
        student[0:rows, columns_of(chunk)] = block[pl.ds(pl.multiple_of(side * rows, rows), rows), :]
        own_store(chunk).start()

    def own_store(chunk):
        spot = columns_of(chunk)
        return pltpu.make_async_copy(student.at[0:rows, spot], own_any.at[:, spot], out_sem.at[0, chunk])

    def pair_store(chunk):
        spot = columns_of(chunk)
        return pltpu.make_async_copy(pair_in.at[:, spot], pair_any.at[:, spot], out_sem.at[1, chunk])

    def early_sums(chunk):
        @pl.loop(0, line - 2)
        def _(index):
            part = jnp.where(next_low, line - 1 - index, index)
            sum_into_block(part, chunk, True)
            send_sum(
                chunk, part, jnp.where(next_low, up, down), jnp.where(next_low, up_slot(part), part), None
            )

    def late_sums(chunk):
        @pl.when(place >= 2)
        def _():
            @pl.loop(0, line - 1 - place)
            def _(index):
                part = line - 1 - index
                sum_into_block(part, chunk, False)
                send_sum(chunk, part, up, up_slot(part), (from_below, base_slot(place) + part - place))

        @pl.when(place <= line - 3)
        def _():
            @pl.loop(0, place)
            def _(part):
                sum_into_block(part, chunk, False)
                send_sum(chunk, part, down, part, (from_above, part))

        sum_into_block(place, chunk, is_next)

        @pl.when(from_below)
        def _():
            add_incoming(chunk, base_slot(place))

        @pl.when(from_above)
        def _():
            add_incoming(chunk, place)

        settle(chunk)

    def drain():
        for part in every:
            for step in range(1, chips):
                gather_far(step, part).wait_send()
                gather_pass(step, part).wait_send()
            gather_copy(0, part, v, other_core).wait_send()
            for step in range(1, vocab):
                stat_copy(step, part, v, lax.rem(v + step, vocab)).wait_send()
            for step in range(chips):
                feature_y(step, part).wait_send()
                feature_core(1, step, part).wait_send()

            @pl.when(is_end)
            def _():
                for which in range(2):
                    feature_z(which, part).wait_send()
                if part == 0:
                    for step in range(1, chips):
                        feature_z_far(step).wait_send()

            @pl.when(is_next)
            def _():
                for which in (2, 3):
                    feature_core(which, 0, part).wait_send()
                    for step in range(1, chips):
                        if which == 2 or part > 0:
                            feature_x(which, step, part).wait_send()
                        feature_core(which, step, part).wait_send()

        @pl.loop(0, chunks)
        def _(chunk):
            for part in every:
                y_copy(part, chunk).wait_send()

        @pl.when(is_end)
        def _():
            @pl.loop(0, chunks)
            def _(chunk):
                for part in every:
                    end_own(part, chunk).wait_send()
                    end_pair(part, chunk).wait_send()

    @pl.loop(0, chunks + plan.last_lag)
    def _(step):
        @pl.when(step < plan.hid_blocks)
        def _():
            hid_block(step)

        if plan.hid_blocks < chunks + plan.last_lag:
            pl.when(step == max(plan.hid_blocks, chunks))(hid_finish)

        pl.when(step == chunks + plan.lag - 1)(drain)

        @pl.when(step < chunks)
        def _():
            for part in range(plan.halves):
                y_copy(part, step).wait_recv()
                pl.when(is_end)(end_pair(part, step).start)

            @pl.when(is_end)
            def _():
                @pl.when(step + plan.ahead < chunks)
                def _():
                    for part in range(plan.halves):
                        end_own(part, step + plan.ahead).start()

            @pl.when(is_next)
            def _():
                for part in range(plan.halves):
                    end_own(part, step).wait_recv()
                    end_pair(part, step).wait_recv()
                early_sums(step)

        @pl.when(
            jnp.logical_and(
                jnp.logical_not(is_end),
                jnp.logical_and(step >= plan.lag, step < chunks + plan.lag),
            )
        )
        def _():
            late_sums(step - plan.lag)

        @pl.when(
            jnp.logical_and(is_end, jnp.logical_and(step >= plan.end_lag, step < chunks + plan.end_lag))
        )
        def _():
            chunk = step - plan.end_lag
            sum_into_block(place, chunk, False)
            add_incoming(chunk, 0)
            settle(chunk)

        @pl.when(step >= plan.last_lag)
        def _():
            chunk = step - plan.last_lag
            last_copy(chunk).wait_recv()
            pair_store(chunk).start()

    @pl.loop(min(chunks + plan.last_lag, plan.hid_blocks), plan.hid_blocks)
    def _(index):
        hid_block(index)

    if plan.hid_blocks >= chunks + plan.last_lag:
        hid_finish()

    hid_store.wait()
    kl_store.wait()

    @pl.loop(0, chunks)
    def _(chunk):
        last_copy(chunk).wait_send()
        own_store(chunk).wait()
        pair_store(chunk).wait()

    @pl.when(jnp.logical_not(is_end))
    def _():
        @pl.loop(chunks - plan.window, chunks)
        def _(chunk):
            @pl.loop(0, place)
            def _(part):
                line_copy(chunk, part, 0, down).wait_send()

            @pl.loop(place + 1, line)
            def _(part):
                line_copy(chunk, part, 0, up).wait_send()


def place_results(
    pieces,
    kl_any, hid_any, own_any, pair_any, kl_out, hid_out, out_ref,
    kl, hid, own, pair, wide, small_sem, big_sem,
):
    side = lax.axis_index("dp") % PAIR
    rows, half = own.shape
    step = rows // pieces

    def load(which, piece):
        where = pl.ds(piece * step, step)
        source, target = ((own_any, own), (pair_any, pair))[which]
        return pltpu.make_async_copy(source.at[where, :], target.at[where, :], big_sem.at[0, which, piece])

    def store(which, piece):
        where = pl.ds(piece * step, step)
        first = (side if which == 0 else PAIR - 1 - side) * half
        return pltpu.make_async_copy(
            (own, wide)[which].at[where, :],
            out_ref.at[where, pl.ds(pl.multiple_of(first, half), half)],
            big_sem.at[1, which, piece],
        )

    small = [
        [pltpu.make_async_copy(kl_any, kl, small_sem.at[0, 0]), pltpu.make_async_copy(kl, kl_out, small_sem.at[1, 0])],
        [pltpu.make_async_copy(hid_any, hid, small_sem.at[0, 1]), pltpu.make_async_copy(hid, hid_out, small_sem.at[1, 1])],
    ]
    for piece in range(pieces):
        for which in (1, 0):
            load(which, piece).start()
    for come, _ in small:
        come.start()
    for piece in range(pieces):
        load(1, piece).wait()
        where = pl.ds(piece * step, step)
        wide[where, :] = pair[where, :].astype(f32)
        store(1, piece).start()
        load(0, piece).wait()
        store(0, piece).start()
    for come, leave in small:
        come.wait()
        leave.start()
    for piece in range(pieces):
        for which in range(2):
            store(which, piece).wait()
    for _, leave in small:
        leave.wait()


def per_device(shards, vocab, hidden_states, teacher_logits, head_weight):
    tokens, shard = hidden_states.shape
    model_width, columns = head_weight.shape
    plan = Plan(shards, vocab, tokens, shard, model_width, columns)
    dma = pltpu.SemaphoreType.DMA
    chips, halves, chunks = plan.chips, plan.halves, plan.chunks
    any_space = pl.BlockSpec(memory_space=pl.ANY)
    divergence, hidden_grad, own_grad, pair_grad = pl.pallas_call(
        functools.partial(fused_kernel, plan),
        out_shape=(
            jax.ShapeDtypeStruct((1, tokens), f32),
            jax.ShapeDtypeStruct((tokens, shard), bf16),
            jax.ShapeDtypeStruct((plan.rows, plan.half), f32),
            jax.ShapeDtypeStruct((plan.rows, plan.half), bf16),
        ),
        in_specs=[any_space] * 3,
        out_specs=(any_space,) * 4,
        scratch_shapes=[
            pltpu.VMEM((1, tokens), f32),
            pltpu.VMEM((tokens, shard), bf16),
            pltpu.VMEM((model_width, columns), bf16),
            pltpu.VMEM((tokens, columns), f32),
            pltpu.VMEM((tokens, columns), bf16),
            pltpu.VMEM((tokens, model_width), bf16),
            pltpu.VMEM((model_width, 4 * tokens), bf16),
            pltpu.VMEM((3 * tokens, plan.half), bf16),
            pltpu.VMEM((plan.slots, plan.rows2, plan.half), bf16),
            pltpu.VMEM((plan.window, plan.line, plan.rows2, plan.width), bf16),
            pltpu.VMEM((plan.rows2, plan.width), f32),
            pltpu.VMEM((plan.rows, plan.half), bf16),
            pltpu.VMEM((plan.rows, plan.half), bf16),
            pltpu.VMEM((chips, tokens, shard), bf16),
            pltpu.VMEM((chips, tokens, shard), bf16),
            pltpu.VMEM((chips - 1, tokens, shard), bf16),
            pltpu.VMEM((chips - 1, tokens, shard), bf16),
            pltpu.VMEM((tokens, shard), f32),
            pltpu.VMEM((tokens, LANES), f32),
            pltpu.VMEM((tokens, LANES), f32),
            pltpu.VMEM((3, tokens, LANES), f32),
            pltpu.VMEM((vocab, 8, tokens), f32),
            dma((4,)), dma((chips, columns // plan.dot_width)), dma((2, chunks)),
            dma((2 * chips - 1, halves)), dma((2 * chips - 1, halves)),
            dma((chips, halves)), dma((chips, halves)),
            dma((2, halves)), dma((2, halves)),
            dma((chips,)), dma((chips,)),
            dma((2, chips, halves)), dma((2, chips, halves)),
            dma((3, chips, halves)), dma((3, chips, halves)),
            dma((vocab, halves)), dma((vocab, halves)),
            dma((halves, chunks)), dma((halves, chunks)),
            dma((halves, chunks)), dma((halves, chunks)),
            dma((halves, chunks)), dma((halves, chunks)),
            dma((plan.line, chunks)), dma((plan.slots, chunks)),
            dma((chunks,)), dma((chunks,)),
            dma((chips,)), dma((chips,)),
            dma((chips - 1,)), dma((chips - 1,)),
        ],
        compiler_params=pltpu.CompilerParams(
            collective_id=0, has_side_effects=True, vmem_limit_bytes=67043328
        ),
    )(hidden_states, teacher_logits, head_weight)
    pieces = 4
    divergence, hidden_grad, head_grad = pl.pallas_call(
        functools.partial(place_results, pieces),
        out_shape=(
            jax.ShapeDtypeStruct((1, tokens), f32),
            jax.ShapeDtypeStruct((tokens, shard), bf16),
            jax.ShapeDtypeStruct((plan.rows, columns), f32),
        ),
        in_specs=[any_space] * 4,
        out_specs=(any_space,) * 3,
        scratch_shapes=[
            pltpu.VMEM((1, tokens), f32),
            pltpu.VMEM((tokens, shard), bf16),
            pltpu.VMEM((plan.rows, plan.half), f32),
            pltpu.VMEM((plan.rows, plan.half), bf16),
            pltpu.VMEM((plan.rows, plan.half), f32),
            dma((2, 2)), dma((2, 2, pieces)),
        ],
        compiler_params=pltpu.CompilerParams(vmem_limit_bytes=16 * 1024 * 1024),
    )(divergence, hidden_grad, own_grad, pair_grad)
    return divergence.reshape(tokens), hidden_grad, head_grad


def solution(mesh):
    in_specs = (P("dp", "vocab"), P("dp", "vocab"), P(None, "vocab"))
    out_specs = (P("dp"), P("dp", "vocab"), P("dp", "vocab"))
    return jax.shard_map(
        functools.partial(per_device, mesh.shape["dp"], mesh.shape["vocab"]),
        mesh=mesh, in_specs=in_specs, out_specs=out_specs, check_vma=False,
    )
```

```python
import functools
import math

import jax
import jax.numpy as jnp
from jax import lax
from jax.experimental import pallas as pl
from jax.experimental.pallas import tpu as pltpu
from jax.sharding import PartitionSpec as P

grad_scale = 8.0
PAIR = 2
CORES = 2
LANES = 128
MESH = pl.DeviceIdType.MESH
f32 = jnp.float32
bf16 = jnp.bfloat16


class Plan:
    def __init__(self, shards, vocab, tokens, shard, model_width, columns):
        self.line = shards // PAIR
        self.vocab = vocab
        self.chips = vocab // CORES
        self.tokens = tokens
        self.shard = shard
        self.model_width = model_width
        self.columns = columns
        self.halves = 2
        self.half_tokens = tokens // self.halves
        self.half_shard = shard // self.halves
        self.half = columns // PAIR
        self.width = min(128, self.half)
        self.chunks = self.half // self.width
        self.rows2 = model_width // self.line
        self.rows = self.rows2 // PAIR
        self.window = min(6, self.chunks)
        self.dot_width = min(512, columns)
        self.lag = 2
        self.end_lag = self.lag + 2
        self.last_lag = max(self.end_lag + 1, self.chunks // 2 + 2)
        self.ahead = 1
        self.first = 1
        self.hid_width = min(256, shard)
        self.hid_subs = shard // self.hid_width
        self.hid_blocks = vocab * self.hid_subs
        self.slots = 2 if self.line == 4 else self.line + 1


def fused_kernel(
    plan,
    hidden_ref, teacher_ref, weight_ref,
    kl_any, hid_any, own_any, pair_any,
    kl_ref, hid_ref, weight, student, grad, gathered, features, pair_grad, incoming, outgoing, block,
    pair_out, pair_in, hid_out, hid_in, hid_far_out, hid_far_in, hid_sum,
    row_student, row_teacher, lane_stats, stats,
    load_sem, weight_sem, out_sem,
    gather_send, gather_recv, fy_send, fy_recv, fz_send, fz_recv, fzf_send, fzf_recv, fx_send, fx_recv, fc_send, fc_recv,
    stat_send, stat_recv, y_send, y_recv, zo_send, zo_recv, zf_send, zf_recv,
    line_send, line_recv, last_send, last_recv,
    hc_send, hc_recv, hx_send, hx_recv,
):
    line, vocab, chips = plan.line, plan.vocab, plan.chips
    tokens, shard, half, width, chunks = plan.tokens, plan.shard, plan.half, plan.width, plan.chunks
    rows2, rows, half_tokens = plan.rows2, plan.rows, plan.half_tokens
    columns = plan.columns

    me = lax.axis_index("dp")
    v = lax.axis_index("vocab")
    place = me // PAIR
    side = me - place * PAIR
    partner = place * PAIR + (PAIR - 1) - side
    chip = v // CORES
    core = v - chip * CORES
    other_core = chip * CORES + (CORES - 1) - core
    has_down = place > 0
    has_up = place < line - 1
    up = jnp.where(has_up, me + PAIR, me)
    down = jnp.where(has_down, me - PAIR, me)
    is_low = place == 0
    is_high = place == line - 1
    is_end = jnp.logical_or(is_low, is_high)
    next_low = place == 1
    next_high = place == line - 2
    is_next = jnp.logical_or(next_low, next_high)
    inner = jnp.where(is_low, up, down)

    def chip_after(step):
        return lax.rem(chip + step, chips)

    def chip_before(step):
        return lax.rem(chip + chips - step, chips)

    def shard_of(index):
        return pl.ds(pl.multiple_of(index * shard, shard), shard)

    def chip_rows(index):
        return pl.ds(pl.multiple_of(index * CORES * shard, CORES * shard), CORES * shard)

    def token_half(part):
        return pl.ds(part * half_tokens, half_tokens)

    def columns_of(chunk):
        return pl.ds(pl.multiple_of(chunk * width, width), width)

    def grad_columns(which, chunk):
        return pl.ds(pl.multiple_of(which * half + chunk * width, width), width)

    def remote(src, dst, send, recv, **target):
        return pltpu.make_async_remote_copy(
            src_ref=src, dst_ref=dst, send_sem=send, recv_sem=recv, device_id=target, device_id_type=MESH
        )

    own_load = pltpu.make_async_copy(hidden_ref, gathered.at[:, shard_of(v)], load_sem.at[0])
    teacher_load = pltpu.make_async_copy(teacher_ref, grad, load_sem.at[1])

    dot_width = plan.dot_width
    dot_blocks = columns // dot_width

    def dot_columns(index):
        return pl.ds(pl.multiple_of(index * dot_width, dot_width), dot_width)

    def weight_load(step, index):
        spot = (chip_rows(chip_before(step)), dot_columns(index))
        return pltpu.make_async_copy(weight_ref.at[spot], weight.at[spot], weight_sem.at[step, index])

    def load_weights(step):
        @pl.loop(0, dot_blocks)
        def _(index):
            weight_load(step, index).start()

    barrier = pltpu.get_barrier_semaphore()
    for step in range(1, vocab):
        pl.semaphore_signal(
            barrier, inc=1, device_id={"vocab": lax.rem(v + step, vocab)}, device_id_type=MESH
        )
    pl.semaphore_signal(barrier, inc=1, device_id={"dp": partner}, device_id_type=MESH)

    @pl.when(has_down)
    def _():
        pl.semaphore_signal(barrier, inc=1, device_id={"dp": down}, device_id_type=MESH)

    @pl.when(has_up)
    def _():
        pl.semaphore_signal(barrier, inc=1, device_id={"dp": up}, device_id_type=MESH)

    own_load.start()
    load_weights(0)
    teacher_load.start()
    for step in range(1, chips):
        load_weights(step)
    own_load.wait()
    pl.semaphore_wait(barrier, vocab + has_down.astype(jnp.int32) + has_up.astype(jnp.int32))

    half_shard = plan.half_shard

    def shard_half(index, part):
        return pl.ds(pl.multiple_of(index * shard + part * half_shard, half_shard), half_shard)

    def gather_copy(index, part, column, target):
        ref = gathered.at[:, shard_half(column, part)]
        return remote(ref, ref, gather_send.at[index, part], gather_recv.at[index, part], vocab=target)

    def gather_far(step, part):
        return gather_copy(step, part, v, chip_after(step) * CORES + core)

    def gather_pass(step, part):
        return gather_copy(chips - 1 + step, part, chip_before(step) * CORES + core, other_core)

    for part in range(plan.halves):
        for step in range(1, chips):
            gather_far(step, part).start()
        gather_copy(0, part, v, other_core).start()

    def set_ref(which, index, part):
        return features.at[shard_half(index, part), pl.ds(which * tokens, tokens)]

    def turn(index, part):
        features[shard_half(index, part), 0:tokens] = gathered[:, shard_half(index, part)].T

    def feature_y(step, part):
        index = chip_before(step) * CORES + core
        return remote(
            set_ref(0, index, part), set_ref(1, index, part), fy_send.at[step, part], fy_recv.at[step, part],
            dp=partner,
        )

    def feature_z(which, part):
        return remote(
            set_ref(which, v, part), set_ref(2 + which, v, part), fz_send.at[which, part], fz_recv.at[which, part],
            dp=inner,
        )

    def feature_z_far(step):
        index = chip_before(step) * CORES + core
        return remote(set_ref(1, index, 0), set_ref(3, index, 0), fzf_send.at[step], fzf_recv.at[step], dp=inner)

    def feature_x(which, step, part):
        ref = set_ref(which, v, part)
        return remote(
            ref, ref, fx_send.at[which - 2, step, part], fx_recv.at[which - 2, step, part],
            vocab=chip_after(step) * CORES + core,
        )

    def feature_core(which, step, part):
        ref = set_ref(which, chip_before(step) * CORES + core, part)
        return remote(
            ref, ref, fc_send.at[which - 1, step, part], fc_recv.at[which - 1, step, part], vocab=other_core
        )

    for part in range(plan.halves):
        turn(v, part)
        feature_y(0, part).start()

        @pl.when(is_end)
        def _():
            feature_z(0, part).start()

    for part in range(plan.halves):
        gather_copy(0, part, other_core, other_core).wait_recv()

    def local_logits():
        @pl.loop(0, dot_blocks)
        def _(index):
            where = dot_columns(index)
            weight_load(0, index).wait()
            student[:, where] = jnp.dot(
                gathered[:, chip_rows(chip)], weight[chip_rows(chip), where], preferred_element_type=f32
            )

    band = 32

    def teacher_tops():
        @pl.loop(0, tokens // band)
        def _(index):
            where = pl.ds(pl.multiple_of(index * band, band), band)
            top = grad[where, 0:LANES]
            for column in range(1, columns // LANES):
                top = jnp.maximum(top, grad[where, column * LANES : (column + 1) * LANES])
            lane_stats[0, where, :] = top.astype(f32)

        row_teacher[...] = jnp.broadcast_to(jnp.max(lane_stats[0], axis=1, keepdims=True), (tokens, LANES))

    local_logits()
    teacher_load.wait()
    teacher_tops()
    for part in range(plan.halves):
        turn(other_core, part)

    def stat_copy(step, part, owner, target):
        ref = stats.at[owner, :, token_half(part)]
        return remote(ref, ref, stat_send.at[step, part], stat_recv.at[step, part], vocab=target)

    def await_far(part):
        for step in range(1, chips):
            gather_copy(
                chips - 1 + step, part, chip_before(step) * CORES + (CORES - 1) - core, other_core
            ).wait_recv()

    def far_logits(part):
        last = part == plan.halves - 1
        if last:
            lane_stats[0] = jnp.full((tokens, LANES), -jnp.inf, f32)

        @pl.loop(0, dot_blocks)
        def _(index):
            where = dot_columns(index)
            total = student[:, where]
            for step in range(1, chips):
                far = [chip_before(step) * CORES + each for each in range(CORES)]
                if part == 0:
                    weight_load(step, index).wait()
                total = total + jnp.dot(
                    jnp.concatenate([gathered[:, shard_half(each, part)] for each in far], axis=1),
                    jnp.concatenate([weight[shard_half(each, part), where] for each in far], axis=0),
                    preferred_element_type=f32,
                )
            student[:, where] = total
            if last:
                top = lane_stats[0]
                for column in range(dot_width // LANES):
                    top = jnp.maximum(top, total[:, column * LANES : (column + 1) * LANES])
                lane_stats[0] = top

    def student_tops(part):
        where_rows = token_half(part)
        student_top = jnp.max(lane_stats[0, where_rows, :], axis=1, keepdims=True)
        row_student[where_rows, :] = jnp.broadcast_to(student_top, (half_tokens, LANES))

    def row_sums(part):
        @pl.loop(0, half_tokens // band)
        def _(index):
            where = pl.ds(pl.multiple_of(part * half_tokens + index * band, band), band)
            student_max, teacher_max = row_student[where, :], row_teacher[where, :]
            sums = [jnp.zeros((band, LANES), f32) for _ in range(3)]
            for column in range(columns // LANES):
                lanes = slice(column * LANES, (column + 1) * LANES)
                logit, target = student[where, lanes], grad[where, lanes].astype(f32)
                term = jnp.exp(target - teacher_max)
                student_term = jnp.exp(logit - student_max)
                student[where, lanes] = student_term
                sums[0] += student_term
                sums[1] += term
                sums[2] += term * (target - logit)
            for which in range(3):
                lane_stats[which, where, :] = sums[which]

    def send_stats(part):
        where_rows = token_half(part)
        lane = lax.broadcasted_iota(jnp.int32, (half_tokens, LANES), 1)
        packed = jnp.where(lane == 0, row_student[where_rows, :], row_teacher[where_rows, :])
        for which in range(3):
            total = jnp.sum(lane_stats[which, where_rows, :], axis=1, keepdims=True)
            packed = jnp.where(lane == 2 + which, jnp.broadcast_to(total, packed.shape), packed)
        stats[v, :, where_rows] = packed.T[0:8, :]
        for step in range(1, vocab):
            stat_copy(step, part, v, lax.rem(v + step, vocab)).start()

    def pass_on(part):
        for step in range(1, chips):
            gather_copy(step, part, chip_before(step) * CORES + core, other_core).wait_recv()
            gather_pass(step, part).start()

    def y_copy(part, chunk):
        return remote(
            grad.at[token_half(part), grad_columns(PAIR - 1 - side, chunk)],
            pair_grad.at[token_half(part), columns_of(chunk)],
            y_send.at[part, chunk], y_recv.at[part, chunk], dp=partner,
        )

    def end_own(part, chunk):
        return remote(
            grad.at[token_half(part), grad_columns(side, chunk)],
            pair_grad.at[pl.ds(tokens + part * half_tokens, half_tokens), columns_of(chunk)],
            zo_send.at[part, chunk], zo_recv.at[part, chunk], dp=inner,
        )

    def end_pair(part, chunk):
        return remote(
            pair_grad.at[token_half(part), columns_of(chunk)],
            pair_grad.at[pl.ds(2 * tokens + part * half_tokens, half_tokens), columns_of(chunk)],
            zf_send.at[part, chunk], zf_recv.at[part, chunk], dp=inner,
        )

    def combine(part):
        where_rows = token_half(part)
        for step in range(1, vocab):
            stat_copy(step, part, lax.rem(v + vocab - step, vocab), other_core).wait_recv()
        parts = [stats[index, :, where_rows] for index in range(vocab)]
        student_max = functools.reduce(jnp.maximum, [p[0:1] for p in parts])
        teacher_max = functools.reduce(jnp.maximum, [p[1:2] for p in parts])
        student_total = sum(p[2:3] * jnp.exp(p[0:1] - student_max) for p in parts)
        teacher_scales = [jnp.exp(p[1:2] - teacher_max) for p in parts]
        teacher_total = sum(p[3:4] * scale for p, scale in zip(parts, teacher_scales))
        cross = sum(p[4:5] * scale for p, scale in zip(parts, teacher_scales))
        student_log = student_max + jnp.log(student_total)
        teacher_log = teacher_max + jnp.log(teacher_total)
        kl_ref[:, where_rows] = cross / teacher_total - teacher_log + student_log
        student_scale = grad_scale * jnp.exp(stats[v, 0:1, where_rows] - student_log)
        row = lax.broadcasted_iota(jnp.int32, (LANES, half_tokens), 0)
        packed = jnp.where(
            row == 0,
            jnp.broadcast_to(student_scale, (LANES, half_tokens)),
            jnp.broadcast_to(teacher_log - math.log(grad_scale), (LANES, half_tokens)),
        ).T
        row_student[where_rows, :] = jnp.broadcast_to(packed[:, 0:1], (half_tokens, LANES))
        row_teacher[where_rows, :] = jnp.broadcast_to(packed[:, 1:2], (half_tokens, LANES))

    def grads(part):
        @pl.loop(0, half_tokens // band)
        def _(index):
            where = pl.ds(pl.multiple_of(part * half_tokens + index * band, band), band)
            student_row, teacher_row = row_student[where, :], row_teacher[where, :]
            for column in range(columns // LANES):
                lanes = slice(column * LANES, (column + 1) * LANES)
                value = student[where, lanes] * student_row - jnp.exp(
                    grad[where, lanes].astype(f32) - teacher_row
                )
                grad[where, lanes] = value.astype(bf16)

    def send_grads(part):
        @pl.loop(0, plan.first)
        def _(chunk):
            y_copy(part, chunk).start()

        @pl.when(is_end)
        def _():
            for chunk in range(plan.ahead):
                end_own(part, chunk).start()

        if part == plan.halves - 1:

            @pl.loop(plan.first, chunks)
            def _(chunk):
                for each in range(plan.halves):
                    y_copy(each, chunk).start()

    def first_service(part):
        feature_y(0, part).wait_recv()
        feature_core(1, 0, part).start()

        @pl.when(is_end)
        def _():
            feature_z(1, part).start()

        @pl.when(is_next)
        def _():
            feature_z(0, part).wait_recv()
            for step in range(1, chips):
                feature_x(2, step, part).start()
            feature_core(2, 0, part).start()

    def turn_far(part):
        for step in range(1, chips):
            turn(chip_before(step) * CORES + core, part)
            feature_y(step, part).start()
        for step in range(1, chips):
            turn(chip_before(step) * CORES + (CORES - 1) - core, part)

    def middle_service(part):
        @pl.when(is_next)
        def _():
            feature_z(1, part).wait_recv()
            if part > 0:
                for step in range(1, chips):
                    feature_x(3, step, part).start()
            feature_core(3, 0, part).start()
            for step in range(1, chips):
                feature_x(2, step, part).wait_recv()
                feature_core(2, step, part).start()

    def second_service(part):
        for step in range(1, chips):
            feature_y(step, part).wait_recv()
            feature_core(1, step, part).start()

            if part == 0:
                pl.when(is_end)(feature_z_far(step).start)

    def last_service(part):
        @pl.when(is_next)
        def _():
            for step in range(1, chips):
                if part > 0:
                    feature_x(3, step, part).wait_recv()
                else:
                    feature_z_far(step).wait_recv()
                feature_core(3, step, part).start()

    def await_features(part):
        for step in range(chips):
            feature_core(1, step, part).wait_recv()

        @pl.when(is_next)
        def _():
            for which in (2, 3):
                for step in range(chips):
                    feature_core(which, step, part).wait_recv()

    every = range(plan.halves)
    for part in every:
        pass_on(part)
        first_service(part)
        await_far(part)
        turn_far(part)
        far_logits(part)
    second_service(0)
    for part in every:
        student_tops(part)
        row_sums(part)
        send_stats(part)
    for part in every:
        middle_service(part)
    for part in every:
        combine(part)
        grads(part)
        send_grads(part)
    for part in every[1:]:
        second_service(part)
    for part in every:
        last_service(part)
    for part in every:
        await_features(part)

    def hid_core(index):
        return remote(
            hid_out.at[index], hid_in.at[index], hc_send.at[index], hc_recv.at[index], vocab=other_core
        )

    def hid_far(index):
        return remote(
            hid_far_out.at[index], hid_far_in.at[index], hx_send.at[index], hx_recv.at[index],
            vocab=lax.rem(chip + 1 + index, chips) * CORES + core,
        )

    def hid_block(index):
        piece = index // plan.hid_subs
        sub = index - piece * plan.hid_subs
        mine = piece >= chips
        order = jnp.where(mine, piece - chips, piece)
        target = lax.rem(chip + 1 + order, chips) * CORES + jnp.where(mine, core, (CORES - 1) - core)
        where = pl.ds(pl.multiple_of(target * shard + sub * plan.hid_width, plan.hid_width), plan.hid_width)
        lanes = pl.ds(pl.multiple_of(sub * plan.hid_width, plan.hid_width), plan.hid_width)
        last_sub = sub == plan.hid_subs - 1
        value = lax.dot_general(
            grad[...], weight[where, :], (((1,), (1,)), ((), ())), preferred_element_type=f32
        )

        @pl.when(jnp.logical_not(mine))
        def _():
            hid_out[order, :, lanes] = value.astype(bf16)

            @pl.when(last_sub)
            def _():
                hid_core(order).start()

        @pl.when(mine)
        def _():
            @pl.when(sub == 0)
            def _():
                hid_core(order).wait_recv()

            total = value + hid_in[order, :, lanes].astype(f32)

            @pl.when(order < chips - 1)
            def _():
                hid_far_out[order, :, lanes] = total.astype(bf16)

                @pl.when(last_sub)
                def _():
                    hid_far(order).start()

            @pl.when(order == chips - 1)
            def _():
                hid_sum[:, lanes] = total

    hid_store = pltpu.make_async_copy(hid_ref, hid_any, load_sem.at[2])
    kl_store = pltpu.make_async_copy(kl_ref, kl_any, load_sem.at[3])
    kl_store.start()

    def hid_finish():
        total = hid_sum[...]
        for index in range(chips - 1):
            hid_far(index).wait_recv()
            total = total + hid_far_in[index].astype(f32)
        hid_ref[...] = total.astype(bf16)
        hid_store.start()
        for step in range(chips):
            hid_core(step).wait_send()
        for index in range(chips - 1):
            hid_far(index).wait_send()

    def rows_of(part):
        return pl.ds(pl.multiple_of(part * rows2, rows2), rows2)

    def sum_into_block(part, chunk, with_end):
        where = columns_of(chunk)
        block[...] = jnp.dot(
            features[rows_of(part), 0:tokens], grad[:, grad_columns(side, chunk)], preferred_element_type=f32
        ) + jnp.dot(
            features[rows_of(part), tokens : 2 * tokens], pair_grad[0:tokens, where], preferred_element_type=f32
        )

        def add_end():
            block[...] += jnp.dot(
                features[rows_of(part), 2 * tokens : 4 * tokens],
                pair_grad[tokens : 3 * tokens, where],
                preferred_element_type=f32,
            )

        if with_end is True:
            add_end()
        elif with_end is not False:
            pl.when(with_end)(add_end)

    def base_slot(where):
        return jnp.where(jnp.logical_and(where >= 1, where <= line - 3), where + 1, 0)

    def line_copy(chunk, part, slot, target):
        return remote(
            outgoing.at[lax.rem(chunk, plan.window), part],
            incoming.at[slot, :, columns_of(chunk)],
            line_send.at[part, chunk], line_recv.at[slot, chunk], dp=target,
        )

    def send_sum(chunk, part, target, slot, source):
        @pl.when(chunk >= plan.window)
        def _():
            line_copy(chunk - plan.window, part, slot, target).wait_send()

        spot = lax.rem(chunk, plan.window)
        if source is None:
            outgoing[spot, part] = block[...].astype(bf16)
        else:
            has_source, source_slot = source

            @pl.when(has_source)
            def _():
                line_copy(chunk, part, source_slot, target).wait_recv()
                outgoing[spot, part] = (
                    block[...] + incoming[source_slot, :, columns_of(chunk)].astype(f32)
                ).astype(bf16)

            @pl.when(jnp.logical_not(has_source))
            def _():
                outgoing[spot, part] = block[...].astype(bf16)

        line_copy(chunk, part, slot, target).start()

    def up_slot(part):
        return base_slot(place + 1) + part - place - 1

    from_below = jnp.logical_and(place >= 2, jnp.logical_not(is_low))
    from_above = place <= line - 3

    def last_copy(chunk):
        return remote(
            pair_out.at[:, columns_of(chunk)], pair_in.at[:, columns_of(chunk)],
            last_send.at[chunk], last_recv.at[chunk], dp=partner,
        )

    def add_incoming(chunk, slot):
        line_copy(chunk, 0, slot, me).wait_recv()
        block[...] += incoming[slot, :, columns_of(chunk)].astype(f32)

    def settle(chunk):
        pair_out[:, columns_of(chunk)] = block[
            pl.ds(pl.multiple_of((PAIR - 1 - side) * rows, rows), rows), :
        ].astype(bf16)
        last_copy(chunk).start()
        student[0:rows, columns_of(chunk)] = block[pl.ds(pl.multiple_of(side * rows, rows), rows), :]
        own_store(chunk).start()

    def own_store(chunk):
        spot = columns_of(chunk)
        return pltpu.make_async_copy(student.at[0:rows, spot], own_any.at[:, spot], out_sem.at[0, chunk])

    def pair_store(chunk):
        spot = columns_of(chunk)
        return pltpu.make_async_copy(pair_in.at[:, spot], pair_any.at[:, spot], out_sem.at[1, chunk])

    def early_sums(chunk):
        @pl.loop(0, line - 2)
        def _(index):
            part = jnp.where(next_low, line - 1 - index, index)
            sum_into_block(part, chunk, True)
            send_sum(
                chunk, part, jnp.where(next_low, up, down), jnp.where(next_low, up_slot(part), part), None
            )

    def late_sums(chunk):
        @pl.when(place >= 2)
        def _():
            @pl.loop(0, line - 1 - place)
            def _(index):
                part = line - 1 - index
                sum_into_block(part, chunk, False)
                send_sum(chunk, part, up, up_slot(part), (from_below, base_slot(place) + part - place))

        @pl.when(place <= line - 3)
        def _():
            @pl.loop(0, place)
            def _(part):
                sum_into_block(part, chunk, False)
                send_sum(chunk, part, down, part, (from_above, part))

        sum_into_block(place, chunk, is_next)

        @pl.when(from_below)
        def _():
            add_incoming(chunk, base_slot(place))

        @pl.when(from_above)
        def _():
            add_incoming(chunk, place)

        settle(chunk)

    def drain():
        for part in every:
            for step in range(1, chips):
                gather_far(step, part).wait_send()
                gather_pass(step, part).wait_send()
            gather_copy(0, part, v, other_core).wait_send()
            for step in range(1, vocab):
                stat_copy(step, part, v, lax.rem(v + step, vocab)).wait_send()
            for step in range(chips):
                feature_y(step, part).wait_send()
                feature_core(1, step, part).wait_send()

            @pl.when(is_end)
            def _():
                for which in range(2):
                    feature_z(which, part).wait_send()
                if part == 0:
                    for step in range(1, chips):
                        feature_z_far(step).wait_send()

            @pl.when(is_next)
            def _():
                for which in (2, 3):
                    feature_core(which, 0, part).wait_send()
                    for step in range(1, chips):
                        if which == 2 or part > 0:
                            feature_x(which, step, part).wait_send()
                        feature_core(which, step, part).wait_send()

        @pl.loop(0, chunks)
        def _(chunk):
            for part in every:
                y_copy(part, chunk).wait_send()

        @pl.when(is_end)
        def _():
            @pl.loop(0, chunks)
            def _(chunk):
                for part in every:
                    end_own(part, chunk).wait_send()
                    end_pair(part, chunk).wait_send()

    def drain_sums():
        kl_store.wait()
        if plan.hid_blocks < chunks + plan.last_lag:
            hid_store.wait()

        @pl.when(jnp.logical_not(is_end))
        def _():
            @pl.loop(chunks - plan.window, chunks)
            def _(chunk):
                @pl.loop(0, place)
                def _(part):
                    line_copy(chunk, part, 0, down).wait_send()

                @pl.loop(place + 1, line)
                def _(part):
                    line_copy(chunk, part, 0, up).wait_send()

    def settled(chunk):
        last_copy(chunk).wait_send()
        own_store(chunk).wait()
        pair_store(chunk).wait()

    @pl.loop(0, chunks + plan.last_lag)
    def _(step):
        pl.when(step == chunks + plan.lag - 1)(drain)

        @pl.when(step < chunks)
        def _():
            for part in range(plan.halves):
                y_copy(part, step).wait_recv()
                pl.when(is_end)(end_pair(part, step).start)

            @pl.when(is_end)
            def _():
                @pl.when(step + plan.ahead < chunks)
                def _():
                    for part in range(plan.halves):
                        end_own(part, step + plan.ahead).start()

            @pl.when(is_next)
            def _():
                for part in range(plan.halves):
                    end_own(part, step).wait_recv()
                    end_pair(part, step).wait_recv()
                early_sums(step)

        @pl.when(
            jnp.logical_and(
                jnp.logical_not(is_end),
                jnp.logical_and(step >= plan.lag, step < chunks + plan.lag),
            )
        )
        def _():
            late_sums(step - plan.lag)

        @pl.when(step < plan.hid_blocks)
        def _():
            hid_block(step)

        if plan.hid_blocks < chunks + plan.last_lag:
            pl.when(step == max(plan.hid_blocks, chunks))(hid_finish)

        @pl.when(
            jnp.logical_and(is_end, jnp.logical_and(step >= plan.end_lag, step < chunks + plan.end_lag))
        )
        def _():
            chunk = step - plan.end_lag
            sum_into_block(place, chunk, False)
            add_incoming(chunk, 0)
            settle(chunk)

        pl.when(step == chunks + plan.last_lag - 1)(drain_sums)

        @pl.when(step >= plan.last_lag)
        def _():
            chunk = step - plan.last_lag
            last_copy(chunk).wait_recv()
            pair_store(chunk).start()

            @pl.when(chunk > 0)
            def _():
                settled(chunk - 1)

    @pl.loop(min(chunks + plan.last_lag, plan.hid_blocks), plan.hid_blocks)
    def _(index):
        hid_block(index)

    if plan.hid_blocks >= chunks + plan.last_lag:
        hid_finish()
        hid_store.wait()

    settled(chunks - 1)


def place_results(
    pieces,
    kl_any, hid_any, own_any, pair_any, kl_out, hid_out, out_ref,
    kl, hid, own, pair, wide, small_sem, big_sem,
):
    side = lax.axis_index("dp") % PAIR
    rows, half = own.shape
    step = rows // pieces

    def load(which, piece):
        where = pl.ds(piece * step, step)
        source, target = ((own_any, own), (pair_any, pair))[which]
        return pltpu.make_async_copy(source.at[where, :], target.at[where, :], big_sem.at[0, which, piece])

    def store(which, piece):
        where = pl.ds(piece * step, step)
        first = (side if which == 0 else PAIR - 1 - side) * half
        return pltpu.make_async_copy(
            (own, wide)[which].at[where, :],
            out_ref.at[where, pl.ds(pl.multiple_of(first, half), half)],
            big_sem.at[1, which, piece],
        )

    small = [
        [pltpu.make_async_copy(kl_any, kl, small_sem.at[0, 0]), pltpu.make_async_copy(kl, kl_out, small_sem.at[1, 0])],
        [pltpu.make_async_copy(hid_any, hid, small_sem.at[0, 1]), pltpu.make_async_copy(hid, hid_out, small_sem.at[1, 1])],
    ]
    for piece in range(pieces):
        for which in (1, 0):
            load(which, piece).start()
    for come, _ in small:
        come.start()
    for piece in range(pieces):
        load(1, piece).wait()
        where = pl.ds(piece * step, step)
        wide[where, :] = pair[where, :].astype(f32)
        store(1, piece).start()
        load(0, piece).wait()
        store(0, piece).start()
    for come, leave in small:
        come.wait()
        leave.start()
    for piece in range(pieces):
        for which in range(2):
            store(which, piece).wait()
    for _, leave in small:
        leave.wait()


def per_device(shards, vocab, hidden_states, teacher_logits, head_weight):
    tokens, shard = hidden_states.shape
    model_width, columns = head_weight.shape
    plan = Plan(shards, vocab, tokens, shard, model_width, columns)
    dma = pltpu.SemaphoreType.DMA
    chips, halves, chunks = plan.chips, plan.halves, plan.chunks
    any_space = pl.BlockSpec(memory_space=pl.ANY)
    divergence, hidden_grad, own_grad, pair_grad = pl.pallas_call(
        functools.partial(fused_kernel, plan),
        out_shape=(
            jax.ShapeDtypeStruct((1, tokens), f32),
            jax.ShapeDtypeStruct((tokens, shard), bf16),
            jax.ShapeDtypeStruct((plan.rows, plan.half), f32),
            jax.ShapeDtypeStruct((plan.rows, plan.half), bf16),
        ),
        in_specs=[any_space] * 3,
        out_specs=(any_space,) * 4,
        scratch_shapes=[
            pltpu.VMEM((1, tokens), f32),
            pltpu.VMEM((tokens, shard), bf16),
            pltpu.VMEM((model_width, columns), bf16),
            pltpu.VMEM((tokens, columns), f32),
            pltpu.VMEM((tokens, columns), bf16),
            pltpu.VMEM((tokens, model_width), bf16),
            pltpu.VMEM((model_width, 4 * tokens), bf16),
            pltpu.VMEM((3 * tokens, plan.half), bf16),
            pltpu.VMEM((plan.slots, plan.rows2, plan.half), bf16),
            pltpu.VMEM((plan.window, plan.line, plan.rows2, plan.width), bf16),
            pltpu.VMEM((plan.rows2, plan.width), f32),
            pltpu.VMEM((plan.rows, plan.half), bf16),
            pltpu.VMEM((plan.rows, plan.half), bf16),
            pltpu.VMEM((chips, tokens, shard), bf16),
            pltpu.VMEM((chips, tokens, shard), bf16),
            pltpu.VMEM((chips - 1, tokens, shard), bf16),
            pltpu.VMEM((chips - 1, tokens, shard), bf16),
            pltpu.VMEM((tokens, shard), f32),
            pltpu.VMEM((tokens, LANES), f32),
            pltpu.VMEM((tokens, LANES), f32),
            pltpu.VMEM((3, tokens, LANES), f32),
            pltpu.VMEM((vocab, 8, tokens), f32),
            dma((4,)), dma((chips, columns // plan.dot_width)), dma((2, chunks)),
            dma((2 * chips - 1, halves)), dma((2 * chips - 1, halves)),
            dma((chips, halves)), dma((chips, halves)),
            dma((2, halves)), dma((2, halves)),
            dma((chips,)), dma((chips,)),
            dma((2, chips, halves)), dma((2, chips, halves)),
            dma((3, chips, halves)), dma((3, chips, halves)),
            dma((vocab, halves)), dma((vocab, halves)),
            dma((halves, chunks)), dma((halves, chunks)),
            dma((halves, chunks)), dma((halves, chunks)),
            dma((halves, chunks)), dma((halves, chunks)),
            dma((plan.line, chunks)), dma((plan.slots, chunks)),
            dma((chunks,)), dma((chunks,)),
            dma((chips,)), dma((chips,)),
            dma((chips - 1,)), dma((chips - 1,)),
        ],
        compiler_params=pltpu.CompilerParams(
            collective_id=0, has_side_effects=True, vmem_limit_bytes=67043328
        ),
    )(hidden_states, teacher_logits, head_weight)
    pieces = 4
    divergence, hidden_grad, head_grad = pl.pallas_call(
        functools.partial(place_results, pieces),
        out_shape=(
            jax.ShapeDtypeStruct((1, tokens), f32),
            jax.ShapeDtypeStruct((tokens, shard), bf16),
            jax.ShapeDtypeStruct((plan.rows, columns), f32),
        ),
        in_specs=[any_space] * 4,
        out_specs=(any_space,) * 3,
        scratch_shapes=[
            pltpu.VMEM((1, tokens), f32),
            pltpu.VMEM((tokens, shard), bf16),
            pltpu.VMEM((plan.rows, plan.half), f32),
            pltpu.VMEM((plan.rows, plan.half), bf16),
            pltpu.VMEM((plan.rows, plan.half), f32),
            dma((2, 2)), dma((2, 2, pieces)),
        ],
        compiler_params=pltpu.CompilerParams(vmem_limit_bytes=67043328),
    )(divergence, hidden_grad, own_grad, pair_grad)
    return divergence.reshape(tokens), hidden_grad, head_grad


def solution(mesh):
    in_specs = (P("dp", "vocab"), P("dp", "vocab"), P(None, "vocab"))
    out_specs = (P("dp"), P("dp", "vocab"), P("dp", "vocab"))
    return jax.shard_map(
        functools.partial(per_device, mesh.shape["dp"], mesh.shape["vocab"]),
        mesh=mesh, in_specs=in_specs, out_specs=out_specs, check_vma=False,
    )
```

```python
import functools
import math

import jax
import jax.numpy as jnp
from jax import lax
from jax.experimental import pallas as pl
from jax.experimental.pallas import tpu as pltpu
from jax.sharding import PartitionSpec as P

grad_scale = 8.0
PAIR = 2
CORES = 2
LANES = 128
MESH = pl.DeviceIdType.MESH
f32 = jnp.float32
bf16 = jnp.bfloat16


class Plan:
    def __init__(self, shards, vocab, tokens, shard, model_width, columns):
        self.line = shards // PAIR
        self.vocab = vocab
        self.chips = vocab // CORES
        self.tokens = tokens
        self.shard = shard
        self.model_width = model_width
        self.columns = columns
        self.halves = 2
        self.half_tokens = tokens // self.halves
        self.half_shard = shard // self.halves
        self.half = columns // PAIR
        self.width = min(128, self.half)
        self.chunks = self.half // self.width
        self.rows2 = model_width // self.line
        self.rows = self.rows2 // PAIR
        self.window = min(6, self.chunks)
        self.dot_width = min(1024, columns)
        self.lag = 2
        self.end_lag = self.lag + 2
        self.last_lag = max(self.end_lag + 1, self.chunks // 2 + 2)
        self.ahead = 1
        self.first = 1
        self.hid_width = min(256, shard)
        self.hid_subs = shard // self.hid_width
        self.hid_blocks = vocab * self.hid_subs
        self.store_lag = min(8, self.chunks)
        self.slots = 2 if self.line == 4 else self.line + 1


def fused_kernel(
    plan,
    hidden_ref, teacher_ref, weight_ref,
    kl_any, hid_any, own_any, pair_any,
    kl_ref, hid_ref, weight, student, grad, gathered, features, pair_grad, incoming, outgoing, block,
    pair_out, pair_in, hid_out, hid_in, hid_far_out, hid_far_in, hid_sum,
    row_student, row_teacher, lane_stats, stats,
    load_sem, weight_sem, out_sem,
    gather_send, gather_recv, fy_send, fy_recv, fz_send, fz_recv, fzf_send, fzf_recv, fx_send, fx_recv, fc_send, fc_recv,
    stat_send, stat_recv, y_send, y_recv, zo_send, zo_recv, zf_send, zf_recv,
    line_send, line_recv, last_send, last_recv,
    hc_send, hc_recv, hx_send, hx_recv,
):
    line, vocab, chips = plan.line, plan.vocab, plan.chips
    tokens, shard, half, width, chunks = plan.tokens, plan.shard, plan.half, plan.width, plan.chunks
    rows2, rows, half_tokens = plan.rows2, plan.rows, plan.half_tokens
    columns = plan.columns

    me = lax.axis_index("dp")
    v = lax.axis_index("vocab")
    place = me // PAIR
    side = me - place * PAIR
    partner = place * PAIR + (PAIR - 1) - side
    chip = v // CORES
    core = v - chip * CORES
    other_core = chip * CORES + (CORES - 1) - core
    has_down = place > 0
    has_up = place < line - 1
    up = jnp.where(has_up, me + PAIR, me)
    down = jnp.where(has_down, me - PAIR, me)
    is_low = place == 0
    is_high = place == line - 1
    is_end = jnp.logical_or(is_low, is_high)
    next_low = place == 1
    next_high = place == line - 2
    is_next = jnp.logical_or(next_low, next_high)
    inner = jnp.where(is_low, up, down)

    def chip_after(step):
        return lax.rem(chip + step, chips)

    def chip_before(step):
        return lax.rem(chip + chips - step, chips)

    def shard_of(index):
        return pl.ds(pl.multiple_of(index * shard, shard), shard)

    def chip_rows(index):
        return pl.ds(pl.multiple_of(index * CORES * shard, CORES * shard), CORES * shard)

    def token_half(part):
        return pl.ds(part * half_tokens, half_tokens)

    def columns_of(chunk):
        return pl.ds(pl.multiple_of(chunk * width, width), width)

    def grad_columns(which, chunk):
        return pl.ds(pl.multiple_of(which * half + chunk * width, width), width)

    def remote(src, dst, send, recv, **target):
        return pltpu.make_async_remote_copy(
            src_ref=src, dst_ref=dst, send_sem=send, recv_sem=recv, device_id=target, device_id_type=MESH
        )

    own_load = pltpu.make_async_copy(hidden_ref, gathered.at[:, shard_of(v)], load_sem.at[0])
    teacher_load = pltpu.make_async_copy(teacher_ref, grad, load_sem.at[1])

    dot_width = plan.dot_width
    dot_blocks = columns // dot_width

    def dot_columns(index):
        return pl.ds(pl.multiple_of(index * dot_width, dot_width), dot_width)

    def weight_load(step, index):
        spot = (chip_rows(chip_before(step)), dot_columns(index))
        return pltpu.make_async_copy(weight_ref.at[spot], weight.at[spot], weight_sem.at[step, index])

    def load_weights(step):
        @pl.loop(0, dot_blocks)
        def _(index):
            weight_load(step, index).start()

    barrier = pltpu.get_barrier_semaphore()
    for step in range(1, vocab):
        pl.semaphore_signal(
            barrier, inc=1, device_id={"vocab": lax.rem(v + step, vocab)}, device_id_type=MESH
        )
    pl.semaphore_signal(barrier, inc=1, device_id={"dp": partner}, device_id_type=MESH)

    @pl.when(has_down)
    def _():
        pl.semaphore_signal(barrier, inc=1, device_id={"dp": down}, device_id_type=MESH)

    @pl.when(has_up)
    def _():
        pl.semaphore_signal(barrier, inc=1, device_id={"dp": up}, device_id_type=MESH)

    own_load.start()
    load_weights(0)
    teacher_load.start()
    for step in range(1, chips):
        load_weights(step)
    own_load.wait()
    pl.semaphore_wait(barrier, vocab + has_down.astype(jnp.int32) + has_up.astype(jnp.int32))

    half_shard = plan.half_shard

    def shard_half(index, part):
        return pl.ds(pl.multiple_of(index * shard + part * half_shard, half_shard), half_shard)

    def gather_copy(index, part, column, target):
        ref = gathered.at[:, shard_half(column, part)]
        return remote(ref, ref, gather_send.at[index, part], gather_recv.at[index, part], vocab=target)

    def gather_far(step, part):
        return gather_copy(step, part, v, chip_after(step) * CORES + core)

    def gather_pass(step, part):
        return gather_copy(chips - 1 + step, part, chip_before(step) * CORES + core, other_core)

    for part in range(plan.halves):
        for step in range(1, chips):
            gather_far(step, part).start()
        gather_copy(0, part, v, other_core).start()

    def set_ref(which, index, part):
        return features.at[shard_half(index, part), pl.ds(which * tokens, tokens)]

    def turn(index, part):
        features[shard_half(index, part), 0:tokens] = gathered[:, shard_half(index, part)].T

    def feature_y(step, part):
        index = chip_before(step) * CORES + core
        return remote(
            set_ref(0, index, part), set_ref(1, index, part), fy_send.at[step, part], fy_recv.at[step, part],
            dp=partner,
        )

    def feature_z(which, part):
        return remote(
            set_ref(which, v, part), set_ref(2 + which, v, part), fz_send.at[which, part], fz_recv.at[which, part],
            dp=inner,
        )

    def feature_z_far(step):
        index = chip_before(step) * CORES + core
        return remote(set_ref(1, index, 0), set_ref(3, index, 0), fzf_send.at[step], fzf_recv.at[step], dp=inner)

    def feature_x(which, step, part):
        ref = set_ref(which, v, part)
        return remote(
            ref, ref, fx_send.at[which - 2, step, part], fx_recv.at[which - 2, step, part],
            vocab=chip_after(step) * CORES + core,
        )

    def feature_core(which, step, part):
        ref = set_ref(which, chip_before(step) * CORES + core, part)
        return remote(
            ref, ref, fc_send.at[which - 1, step, part], fc_recv.at[which - 1, step, part], vocab=other_core
        )

    for part in range(plan.halves):
        turn(v, part)
        feature_y(0, part).start()

        @pl.when(is_end)
        def _():
            feature_z(0, part).start()

    for part in range(plan.halves):
        gather_copy(0, part, other_core, other_core).wait_recv()

    def local_logits():
        @pl.loop(0, dot_blocks)
        def _(index):
            where = dot_columns(index)
            weight_load(0, index).wait()
            student[:, where] = jnp.dot(
                gathered[:, chip_rows(chip)], weight[chip_rows(chip), where], preferred_element_type=f32
            )

    band = 32

    def teacher_tops():
        @pl.loop(0, tokens // band)
        def _(index):
            where = pl.ds(pl.multiple_of(index * band, band), band)
            top = grad[where, 0:LANES]
            for column in range(1, columns // LANES):
                top = jnp.maximum(top, grad[where, column * LANES : (column + 1) * LANES])
            lane_stats[0, where, :] = top.astype(f32)

        row_teacher[...] = jnp.broadcast_to(jnp.max(lane_stats[0], axis=1, keepdims=True), (tokens, LANES))

    local_logits()
    teacher_load.wait()
    teacher_tops()
    for part in range(plan.halves):
        turn(other_core, part)

    def stat_copy(step, part, owner, target):
        ref = stats.at[owner, :, token_half(part)]
        return remote(ref, ref, stat_send.at[step, part], stat_recv.at[step, part], vocab=target)

    def await_far(part):
        for step in range(1, chips):
            gather_copy(
                chips - 1 + step, part, chip_before(step) * CORES + (CORES - 1) - core, other_core
            ).wait_recv()

    def far_logits(part):
        last = part == plan.halves - 1
        if last:
            lane_stats[0] = jnp.full((tokens, LANES), -jnp.inf, f32)

        @pl.loop(0, dot_blocks)
        def _(index):
            where = dot_columns(index)
            total = student[:, where]
            for step in range(1, chips):
                far = [chip_before(step) * CORES + each for each in range(CORES)]
                if part == 0:
                    weight_load(step, index).wait()
                total = total + jnp.dot(
                    jnp.concatenate([gathered[:, shard_half(each, part)] for each in far], axis=1),
                    jnp.concatenate([weight[shard_half(each, part), where] for each in far], axis=0),
                    preferred_element_type=f32,
                )
            student[:, where] = total
            if last:
                top = lane_stats[0]
                for column in range(dot_width // LANES):
                    top = jnp.maximum(top, total[:, column * LANES : (column + 1) * LANES])
                lane_stats[0] = top

    def student_tops(part):
        where_rows = token_half(part)
        student_top = jnp.max(lane_stats[0, where_rows, :], axis=1, keepdims=True)
        row_student[where_rows, :] = jnp.broadcast_to(student_top, (half_tokens, LANES))

    def row_sums(part):
        @pl.loop(0, half_tokens // band)
        def _(index):
            where = pl.ds(pl.multiple_of(part * half_tokens + index * band, band), band)
            student_max, teacher_max = row_student[where, :], row_teacher[where, :]
            sums = [jnp.zeros((band, LANES), f32) for _ in range(3)]
            for column in range(columns // LANES):
                lanes = slice(column * LANES, (column + 1) * LANES)
                logit, target = student[where, lanes], grad[where, lanes].astype(f32)
                term = jnp.exp(target - teacher_max)
                student_term = jnp.exp(logit - student_max)
                student[where, lanes] = student_term
                sums[0] += student_term
                sums[1] += term
                sums[2] += term * (target - logit)
            for which in range(3):
                lane_stats[which, where, :] = sums[which]

    def send_stats(part):
        where_rows = token_half(part)
        lane = lax.broadcasted_iota(jnp.int32, (half_tokens, LANES), 1)
        packed = jnp.where(lane == 0, row_student[where_rows, :], row_teacher[where_rows, :])
        for which in range(3):
            total = jnp.sum(lane_stats[which, where_rows, :], axis=1, keepdims=True)
            packed = jnp.where(lane == 2 + which, jnp.broadcast_to(total, packed.shape), packed)
        stats[v, :, where_rows] = packed.T[0:8, :]
        for step in range(1, vocab):
            stat_copy(step, part, v, lax.rem(v + step, vocab)).start()

    def pass_on(part):
        for step in range(1, chips):
            gather_copy(step, part, chip_before(step) * CORES + core, other_core).wait_recv()
            gather_pass(step, part).start()

    def y_copy(part, chunk):
        return remote(
            grad.at[token_half(part), grad_columns(PAIR - 1 - side, chunk)],
            pair_grad.at[token_half(part), columns_of(chunk)],
            y_send.at[part, chunk], y_recv.at[part, chunk], dp=partner,
        )

    def end_own(part, chunk):
        return remote(
            grad.at[token_half(part), grad_columns(side, chunk)],
            pair_grad.at[pl.ds(tokens + part * half_tokens, half_tokens), columns_of(chunk)],
            zo_send.at[part, chunk], zo_recv.at[part, chunk], dp=inner,
        )

    def end_pair(part, chunk):
        return remote(
            pair_grad.at[token_half(part), columns_of(chunk)],
            pair_grad.at[pl.ds(2 * tokens + part * half_tokens, half_tokens), columns_of(chunk)],
            zf_send.at[part, chunk], zf_recv.at[part, chunk], dp=inner,
        )

    def combine(part):
        where_rows = token_half(part)
        for step in range(1, vocab):
            stat_copy(step, part, lax.rem(v + vocab - step, vocab), other_core).wait_recv()
        parts = [stats[index, :, where_rows] for index in range(vocab)]
        student_max = functools.reduce(jnp.maximum, [p[0:1] for p in parts])
        teacher_max = functools.reduce(jnp.maximum, [p[1:2] for p in parts])
        student_total = sum(p[2:3] * jnp.exp(p[0:1] - student_max) for p in parts)
        teacher_scales = [jnp.exp(p[1:2] - teacher_max) for p in parts]
        teacher_total = sum(p[3:4] * scale for p, scale in zip(parts, teacher_scales))
        cross = sum(p[4:5] * scale for p, scale in zip(parts, teacher_scales))
        student_log = student_max + jnp.log(student_total)
        teacher_log = teacher_max + jnp.log(teacher_total)
        kl_ref[:, where_rows] = cross / teacher_total - teacher_log + student_log
        student_scale = grad_scale * jnp.exp(stats[v, 0:1, where_rows] - student_log)
        row = lax.broadcasted_iota(jnp.int32, (LANES, half_tokens), 0)
        packed = jnp.where(
            row == 0,
            jnp.broadcast_to(student_scale, (LANES, half_tokens)),
            jnp.broadcast_to(teacher_log - math.log(grad_scale), (LANES, half_tokens)),
        ).T
        row_student[where_rows, :] = jnp.broadcast_to(packed[:, 0:1], (half_tokens, LANES))
        row_teacher[where_rows, :] = jnp.broadcast_to(packed[:, 1:2], (half_tokens, LANES))

    def grads(part):
        @pl.loop(0, half_tokens // band)
        def _(index):
            where = pl.ds(pl.multiple_of(part * half_tokens + index * band, band), band)
            student_row, teacher_row = row_student[where, :], row_teacher[where, :]
            for column in range(columns // LANES):
                lanes = slice(column * LANES, (column + 1) * LANES)
                value = student[where, lanes] * student_row - jnp.exp(
                    grad[where, lanes].astype(f32) - teacher_row
                )
                grad[where, lanes] = value.astype(bf16)

    def send_grads(part):
        @pl.loop(0, plan.first)
        def _(chunk):
            y_copy(part, chunk).start()

        @pl.when(is_end)
        def _():
            for chunk in range(plan.ahead):
                end_own(part, chunk).start()

        if part == plan.halves - 1:

            @pl.loop(plan.first, chunks)
            def _(chunk):
                for each in range(plan.halves):
                    y_copy(each, chunk).start()

    def first_service(part):
        feature_y(0, part).wait_recv()
        feature_core(1, 0, part).start()

        @pl.when(is_end)
        def _():
            feature_z(1, part).start()

        @pl.when(is_next)
        def _():
            feature_z(0, part).wait_recv()
            for step in range(1, chips):
                feature_x(2, step, part).start()
            feature_core(2, 0, part).start()

    def turn_far(part):
        for step in range(1, chips):
            turn(chip_before(step) * CORES + core, part)
            feature_y(step, part).start()
        for step in range(1, chips):
            turn(chip_before(step) * CORES + (CORES - 1) - core, part)

    def middle_service(part):
        @pl.when(is_next)
        def _():
            feature_z(1, part).wait_recv()
            if part > 0:
                for step in range(1, chips):
                    feature_x(3, step, part).start()
            feature_core(3, 0, part).start()
            for step in range(1, chips):
                feature_x(2, step, part).wait_recv()
                feature_core(2, step, part).start()

    def second_service(part):
        for step in range(1, chips):
            feature_y(step, part).wait_recv()
            feature_core(1, step, part).start()

            if part == 0:
                pl.when(is_end)(feature_z_far(step).start)

    def last_service(part):
        @pl.when(is_next)
        def _():
            for step in range(1, chips):
                if part > 0:
                    feature_x(3, step, part).wait_recv()
                else:
                    feature_z_far(step).wait_recv()
                feature_core(3, step, part).start()

    def await_features(part):
        for step in range(chips):
            feature_core(1, step, part).wait_recv()

        @pl.when(is_next)
        def _():
            for which in (2, 3):
                for step in range(chips):
                    feature_core(which, step, part).wait_recv()

    every = range(plan.halves)
    for part in every:
        pass_on(part)
        first_service(part)
        await_far(part)
        turn_far(part)
        far_logits(part)
    second_service(0)
    for part in every:
        student_tops(part)
        row_sums(part)
        send_stats(part)
    for part in every:
        middle_service(part)
    for part in every:
        combine(part)
        grads(part)
        send_grads(part)
    for part in every[1:]:
        second_service(part)
    for part in every:
        last_service(part)
    for part in every:
        await_features(part)

    def hid_core(index):
        return remote(
            hid_out.at[index], hid_in.at[index], hc_send.at[index], hc_recv.at[index], vocab=other_core
        )

    def hid_far(index):
        return remote(
            hid_far_out.at[index], hid_far_in.at[index], hx_send.at[index], hx_recv.at[index],
            vocab=lax.rem(chip + 1 + index, chips) * CORES + core,
        )

    def hid_block(index):
        piece = index // plan.hid_subs
        sub = index - piece * plan.hid_subs
        mine = piece >= chips
        order = jnp.where(mine, piece - chips, piece)
        target = lax.rem(chip + 1 + order, chips) * CORES + jnp.where(mine, core, (CORES - 1) - core)
        where = pl.ds(pl.multiple_of(target * shard + sub * plan.hid_width, plan.hid_width), plan.hid_width)
        lanes = pl.ds(pl.multiple_of(sub * plan.hid_width, plan.hid_width), plan.hid_width)
        last_sub = sub == plan.hid_subs - 1
        value = lax.dot_general(
            grad[...], weight[where, :], (((1,), (1,)), ((), ())), preferred_element_type=f32
        )

        @pl.when(jnp.logical_not(mine))
        def _():
            hid_out[order, :, lanes] = value.astype(bf16)

            @pl.when(last_sub)
            def _():
                hid_core(order).start()

        @pl.when(mine)
        def _():
            @pl.when(sub == 0)
            def _():
                hid_core(order).wait_recv()

            total = value + hid_in[order, :, lanes].astype(f32)

            @pl.when(order < chips - 1)
            def _():
                hid_far_out[order, :, lanes] = total.astype(bf16)

                @pl.when(last_sub)
                def _():
                    hid_far(order).start()

            @pl.when(order == chips - 1)
            def _():
                hid_sum[:, lanes] = total

    hid_store = pltpu.make_async_copy(hid_ref, hid_any, load_sem.at[2])
    kl_store = pltpu.make_async_copy(kl_ref, kl_any, load_sem.at[3])
    kl_store.start()

    def hid_finish():
        total = hid_sum[...]
        for index in range(chips - 1):
            hid_far(index).wait_recv()
            total = total + hid_far_in[index].astype(f32)
        hid_ref[...] = total.astype(bf16)
        hid_store.start()
        for step in range(chips):
            hid_core(step).wait_send()
        for index in range(chips - 1):
            hid_far(index).wait_send()

    def rows_of(part):
        return pl.ds(pl.multiple_of(part * rows2, rows2), rows2)

    def sum_into_block(part, chunk, with_end):
        where = columns_of(chunk)
        block[...] = jnp.dot(
            features[rows_of(part), 0:tokens], grad[:, grad_columns(side, chunk)], preferred_element_type=f32
        ) + jnp.dot(
            features[rows_of(part), tokens : 2 * tokens], pair_grad[0:tokens, where], preferred_element_type=f32
        )

        def add_end():
            block[...] += jnp.dot(
                features[rows_of(part), 2 * tokens : 4 * tokens],
                pair_grad[tokens : 3 * tokens, where],
                preferred_element_type=f32,
            )

        if with_end is True:
            add_end()
        elif with_end is not False:
            pl.when(with_end)(add_end)

    def base_slot(where):
        return jnp.where(jnp.logical_and(where >= 1, where <= line - 3), where + 1, 0)

    def line_copy(chunk, part, slot, target):
        return remote(
            outgoing.at[lax.rem(chunk, plan.window), part],
            incoming.at[slot, :, columns_of(chunk)],
            line_send.at[part, lax.rem(chunk, plan.window)], line_recv.at[slot, chunk], dp=target,
        )

    def send_sum(chunk, part, target, slot, source):
        @pl.when(chunk >= plan.window)
        def _():
            line_copy(chunk - plan.window, part, slot, target).wait_send()

        spot = lax.rem(chunk, plan.window)
        if source is None:
            outgoing[spot, part] = block[...].astype(bf16)
        else:
            has_source, source_slot = source

            @pl.when(has_source)
            def _():
                line_copy(chunk, part, source_slot, target).wait_recv()
                outgoing[spot, part] = (
                    block[...] + incoming[source_slot, :, columns_of(chunk)].astype(f32)
                ).astype(bf16)

            @pl.when(jnp.logical_not(has_source))
            def _():
                outgoing[spot, part] = block[...].astype(bf16)

        line_copy(chunk, part, slot, target).start()

    def up_slot(part):
        return base_slot(place + 1) + part - place - 1

    from_below = jnp.logical_and(place >= 2, jnp.logical_not(is_low))
    from_above = place <= line - 3

    def last_copy(chunk):
        return remote(
            pair_out.at[:, columns_of(chunk)], pair_in.at[:, columns_of(chunk)],
            last_send.at[chunk], last_recv.at[chunk], dp=partner,
        )

    def add_incoming(chunk, slot):
        line_copy(chunk, 0, slot, me).wait_recv()
        block[...] += incoming[slot, :, columns_of(chunk)].astype(f32)

    def settle(chunk):
        pair_out[:, columns_of(chunk)] = block[
            pl.ds(pl.multiple_of((PAIR - 1 - side) * rows, rows), rows), :
        ].astype(bf16)
        last_copy(chunk).start()
        student[0:rows, columns_of(chunk)] = block[pl.ds(pl.multiple_of(side * rows, rows), rows), :]
        own_store(chunk).start()

    def own_store(chunk):
        spot = columns_of(chunk)
        return pltpu.make_async_copy(student.at[0:rows, spot], own_any.at[:, spot], out_sem.at[0, chunk])

    def pair_store(chunk):
        spot = columns_of(chunk)
        return pltpu.make_async_copy(pair_in.at[:, spot], pair_any.at[:, spot], out_sem.at[1, chunk])

    def early_sums(chunk):
        @pl.loop(0, line - 2)
        def _(index):
            part = jnp.where(next_low, line - 1 - index, index)
            sum_into_block(part, chunk, True)
            send_sum(
                chunk, part, jnp.where(next_low, up, down), jnp.where(next_low, up_slot(part), part), None
            )

    def late_sums(chunk):
        @pl.when(place >= 2)
        def _():
            @pl.loop(0, line - 1 - place)
            def _(index):
                part = line - 1 - index
                sum_into_block(part, chunk, False)
                send_sum(chunk, part, up, up_slot(part), (from_below, base_slot(place) + part - place))

        @pl.when(place <= line - 3)
        def _():
            @pl.loop(0, place)
            def _(part):
                sum_into_block(part, chunk, False)
                send_sum(chunk, part, down, part, (from_above, part))

        sum_into_block(place, chunk, is_next)

        @pl.when(from_below)
        def _():
            add_incoming(chunk, base_slot(place))

        @pl.when(from_above)
        def _():
            add_incoming(chunk, place)

        settle(chunk)

    def drain():
        for part in every:
            for step in range(1, chips):
                gather_far(step, part).wait_send()
                gather_pass(step, part).wait_send()
            gather_copy(0, part, v, other_core).wait_send()
            for step in range(1, vocab):
                stat_copy(step, part, v, lax.rem(v + step, vocab)).wait_send()
            for step in range(chips):
                feature_y(step, part).wait_send()
                feature_core(1, step, part).wait_send()

            @pl.when(is_end)
            def _():
                for which in range(2):
                    feature_z(which, part).wait_send()
                if part == 0:
                    for step in range(1, chips):
                        feature_z_far(step).wait_send()

            @pl.when(is_next)
            def _():
                for which in (2, 3):
                    feature_core(which, 0, part).wait_send()
                    for step in range(1, chips):
                        if which == 2 or part > 0:
                            feature_x(which, step, part).wait_send()
                        feature_core(which, step, part).wait_send()

        @pl.loop(0, chunks)
        def _(chunk):
            for part in every:
                y_copy(part, chunk).wait_send()

        @pl.when(is_end)
        def _():
            @pl.loop(0, chunks)
            def _(chunk):
                for part in every:
                    end_own(part, chunk).wait_send()
                    end_pair(part, chunk).wait_send()

    def drain_sums():
        kl_store.wait()
        if plan.hid_blocks < chunks + plan.last_lag:
            hid_store.wait()

        @pl.when(jnp.logical_not(is_end))
        def _():
            @pl.loop(chunks - plan.window, chunks)
            def _(chunk):
                @pl.loop(0, place)
                def _(part):
                    line_copy(chunk, part, 0, down).wait_send()

                @pl.loop(place + 1, line)
                def _(part):
                    line_copy(chunk, part, 0, up).wait_send()

    def settled(chunk):
        last_copy(chunk).wait_send()
        own_store(chunk).wait()

    @pl.loop(0, chunks + plan.last_lag)
    def _(step):
        pl.when(step == chunks + plan.lag - 1)(drain)

        @pl.when(step < chunks)
        def _():
            for part in range(plan.halves):
                y_copy(part, step).wait_recv()
                pl.when(is_end)(end_pair(part, step).start)

            @pl.when(is_end)
            def _():
                @pl.when(step + plan.ahead < chunks)
                def _():
                    for part in range(plan.halves):
                        end_own(part, step + plan.ahead).start()

            @pl.when(is_next)
            def _():
                for part in range(plan.halves):
                    end_own(part, step).wait_recv()
                    end_pair(part, step).wait_recv()
                early_sums(step)

        @pl.when(
            jnp.logical_and(
                jnp.logical_not(is_end),
                jnp.logical_and(step >= plan.lag, step < chunks + plan.lag),
            )
        )
        def _():
            late_sums(step - plan.lag)

        @pl.when(step < plan.hid_blocks)
        def _():
            hid_block(step)

        if plan.hid_blocks < chunks + plan.last_lag:
            pl.when(step == max(plan.hid_blocks, chunks))(hid_finish)

        @pl.when(
            jnp.logical_and(is_end, jnp.logical_and(step >= plan.end_lag, step < chunks + plan.end_lag))
        )
        def _():
            chunk = step - plan.end_lag
            sum_into_block(place, chunk, False)
            add_incoming(chunk, 0)
            settle(chunk)

        pl.when(step == chunks + plan.last_lag - 1)(drain_sums)

        @pl.when(step >= plan.last_lag)
        def _():
            chunk = step - plan.last_lag
            last_copy(chunk).wait_recv()
            pair_store(chunk).start()

            @pl.when(chunk > 0)
            def _():
                settled(chunk - 1)

            @pl.when(chunk >= plan.store_lag)
            def _():
                pair_store(chunk - plan.store_lag).wait()

    @pl.loop(min(chunks + plan.last_lag, plan.hid_blocks), plan.hid_blocks)
    def _(index):
        hid_block(index)

    if plan.hid_blocks >= chunks + plan.last_lag:
        hid_finish()
        hid_store.wait()

    settled(chunks - 1)

    @pl.loop(chunks - plan.store_lag, chunks)
    def _(chunk):
        pair_store(chunk).wait()


def place_results(
    pieces,
    kl_any, hid_any, own_any, pair_any, kl_out, hid_out, out_ref,
    kl, hid, own, pair, wide, small_sem, big_sem,
):
    side = lax.axis_index("dp") % PAIR
    rows, half = own.shape
    step = rows // pieces

    def load(which, piece):
        where = pl.ds(piece * step, step)
        source, target = ((own_any, own), (pair_any, pair))[which]
        return pltpu.make_async_copy(source.at[where, :], target.at[where, :], big_sem.at[0, which, piece])

    def store(which, piece):
        where = pl.ds(piece * step, step)
        first = (side if which == 0 else PAIR - 1 - side) * half
        return pltpu.make_async_copy(
            (own, wide)[which].at[where, :],
            out_ref.at[where, pl.ds(pl.multiple_of(first, half), half)],
            big_sem.at[1, which, piece],
        )

    small = [
        [pltpu.make_async_copy(kl_any, kl, small_sem.at[0, 0]), pltpu.make_async_copy(kl, kl_out, small_sem.at[1, 0])],
        [pltpu.make_async_copy(hid_any, hid, small_sem.at[0, 1]), pltpu.make_async_copy(hid, hid_out, small_sem.at[1, 1])],
    ]
    for piece in range(pieces):
        for which in (1, 0):
            load(which, piece).start()
    for come, _ in small:
        come.start()
    for piece in range(pieces):
        load(1, piece).wait()
        where = pl.ds(piece * step, step)
        wide[where, :] = pair[where, :].astype(f32)
        store(1, piece).start()
        load(0, piece).wait()
        store(0, piece).start()
    for come, leave in small:
        come.wait()
        leave.start()
    for piece in range(pieces):
        for which in range(2):
            store(which, piece).wait()
    for _, leave in small:
        leave.wait()


def per_device(shards, vocab, hidden_states, teacher_logits, head_weight):
    tokens, shard = hidden_states.shape
    model_width, columns = head_weight.shape
    plan = Plan(shards, vocab, tokens, shard, model_width, columns)
    dma = pltpu.SemaphoreType.DMA
    chips, halves, chunks = plan.chips, plan.halves, plan.chunks
    any_space = pl.BlockSpec(memory_space=pl.ANY)
    divergence, hidden_grad, own_grad, pair_grad = pl.pallas_call(
        functools.partial(fused_kernel, plan),
        out_shape=(
            jax.ShapeDtypeStruct((1, tokens), f32),
            jax.ShapeDtypeStruct((tokens, shard), bf16),
            jax.ShapeDtypeStruct((plan.rows, plan.half), f32),
            jax.ShapeDtypeStruct((plan.rows, plan.half), bf16),
        ),
        in_specs=[any_space] * 3,
        out_specs=(any_space,) * 4,
        scratch_shapes=[
            pltpu.VMEM((1, tokens), f32),
            pltpu.VMEM((tokens, shard), bf16),
            pltpu.VMEM((model_width, columns), bf16),
            pltpu.VMEM((tokens, columns), f32),
            pltpu.VMEM((tokens, columns), bf16),
            pltpu.VMEM((tokens, model_width), bf16),
            pltpu.VMEM((model_width, 4 * tokens), bf16),
            pltpu.VMEM((3 * tokens, plan.half), bf16),
            pltpu.VMEM((plan.slots, plan.rows2, plan.half), bf16),
            pltpu.VMEM((plan.window, plan.line, plan.rows2, plan.width), bf16),
            pltpu.VMEM((plan.rows2, plan.width), f32),
            pltpu.VMEM((plan.rows, plan.half), bf16),
            pltpu.VMEM((plan.rows, plan.half), bf16),
            pltpu.VMEM((chips, tokens, shard), bf16),
            pltpu.VMEM((chips, tokens, shard), bf16),
            pltpu.VMEM((chips - 1, tokens, shard), bf16),
            pltpu.VMEM((chips - 1, tokens, shard), bf16),
            pltpu.VMEM((tokens, shard), f32),
            pltpu.VMEM((tokens, LANES), f32),
            pltpu.VMEM((tokens, LANES), f32),
            pltpu.VMEM((3, tokens, LANES), f32),
            pltpu.VMEM((vocab, 8, tokens), f32),
            dma((4,)), dma((chips, columns // plan.dot_width)), dma((2, chunks)),
            dma((2 * chips - 1, halves)), dma((2 * chips - 1, halves)),
            dma((chips, halves)), dma((chips, halves)),
            dma((2, halves)), dma((2, halves)),
            dma((chips,)), dma((chips,)),
            dma((2, chips, halves)), dma((2, chips, halves)),
            dma((3, chips, halves)), dma((3, chips, halves)),
            dma((vocab, halves)), dma((vocab, halves)),
            dma((halves, chunks)), dma((halves, chunks)),
            dma((halves, chunks)), dma((halves, chunks)),
            dma((halves, chunks)), dma((halves, chunks)),
            dma((plan.line, plan.window)), dma((plan.slots, chunks)),
            dma((chunks,)), dma((chunks,)),
            dma((chips,)), dma((chips,)),
            dma((chips - 1,)), dma((chips - 1,)),
        ],
        compiler_params=pltpu.CompilerParams(
            collective_id=0, has_side_effects=True, vmem_limit_bytes=67043328
        ),
    )(hidden_states, teacher_logits, head_weight)
    pieces = 4
    divergence, hidden_grad, head_grad = pl.pallas_call(
        functools.partial(place_results, pieces),
        out_shape=(
            jax.ShapeDtypeStruct((1, tokens), f32),
            jax.ShapeDtypeStruct((tokens, shard), bf16),
            jax.ShapeDtypeStruct((plan.rows, columns), f32),
        ),
        in_specs=[any_space] * 4,
        out_specs=(any_space,) * 3,
        scratch_shapes=[
            pltpu.VMEM((1, tokens), f32),
            pltpu.VMEM((tokens, shard), bf16),
            pltpu.VMEM((plan.rows, plan.half), f32),
            pltpu.VMEM((plan.rows, plan.half), bf16),
            pltpu.VMEM((plan.rows, plan.half), f32),
            dma((2, 2)), dma((2, 2, pieces)),
        ],
        compiler_params=pltpu.CompilerParams(vmem_limit_bytes=67043328),
    )(divergence, hidden_grad, own_grad, pair_grad)
    return divergence.reshape(tokens), hidden_grad, head_grad


def solution(mesh):
    in_specs = (P("dp", "vocab"), P("dp", "vocab"), P(None, "vocab"))
    out_specs = (P("dp"), P("dp", "vocab"), P("dp", "vocab"))
    return jax.shard_map(
        functools.partial(per_device, mesh.shape["dp"], mesh.shape["vocab"]),
        mesh=mesh, in_specs=in_specs, out_specs=out_specs, check_vma=False,
    )
```
